32 devices in a mesh: tensor: 4 (over x, core), dp: 8 (over z, y).
Axes of the slice: x: 2, y: 2, z: 4, core: 2. Of those that a mesh axis runs over, the one named last changes fastest.
Arguments:
- grads: bfloat16 [8, 4, 8192, 1024], P('dp', None, None, 'tensor'), may hold values from -6 to 6
- param: float32 [4, 8192, 1024], P(None, 'dp', 'tensor'), may hold values from -3 to 3
- q_m: bfloat16 [4, 8192, 1024], P(None, 'dp', 'tensor'), may hold values from -1 to 1
- m_scale: float32 [4], replicated, may hold values from 0.02 to 0.2
- q_v: bfloat16 [4, 8192, 1024], P(None, 'dp', 'tensor'), may hold values from 0.0009994507 to 1
- v_max: float32 [4, 8], P(None, 'tensor'), may hold values from 0.005 to 0.05
- v_exp: float32 [4, 8], P(None, 'tensor'), may hold values from 1 to 10
Outputs:
- new_param: float32 [4, 8192, 1024], P(None, 'dp', 'tensor')
- new_q_m: bfloat16 [4, 8192, 1024], P(None, 'dp', 'tensor')
- new_m_scale: float32 [4], replicated
- new_q_v: bfloat16 [4, 8192, 1024], P(None, 'dp', 'tensor')
- new_v_max: float32 [4, 8], P(None, 'tensor')
- new_v_exp: float32 [4, 8], P(None, 'tensor')
The draws below stay inside these ranges and needn't reach their ends.
All inputs are finite; a program needn't handle non-finite values. Where the reference program divides by a largest or mean magnitude, that divisor is 1e-20 or more.
Results may differ from the reference program's by a relative error of at most 0.001.
Values sent between devices are 32-bit elements; how exact they have to be, the bound alone decides.
A program may use at most 192 MiB of HBM per device.

```python
import math
import jax
import jax.numpy as jnp
from jax import lax

D = 8192
KVW = 1024
HEAD = 128
TENSORS = 4
GROUPS = 8
REPLICAS = 8


def with_spikes(result, rng, source, target, parts, factor):
    def block_of(position):
        return (jnp.arange(result.shape[position]) // (result.shape[position] // parts)).reshape((-1,) + (1,) * (result.ndim - 1 - position))

    one_side = jax.random.permutation(rng, parts)[block_of(target)]
    second = (block_of(target) + parts // 2) % parts
    return jnp.where((block_of(source) == one_side) | (block_of(source) == second), factor * result, result)


def shard_levels(stream_key, dims, split, smallest, largest):
    loudness, own = 1.0, jax.random.fold_in(stream_key, 6)
    for axis_at, shards_of in split:
        steps = jnp.exp(jax.random.uniform(jax.random.fold_in(own, axis_at), (shards_of,), jnp.float32, smallest / len(split), largest / len(split)))
        loudness = loudness * jnp.repeat(steps, dims[axis_at] // shards_of).reshape([-1 if axis == axis_at else 1 for axis in range(len(dims))])
    return loudness


def gaussian(rng, shape, deviation, most, pieces=(), kind=jnp.bfloat16):
    values = jax.random.normal(rng, shape, jnp.float32) * deviation
    if len(pieces) > 0:
        values = shard_levels(rng, shape, pieces, -0.22, 0.18) * values
    return jnp.clip(values, min=-most, max=most).astype(kind)


def heavy_noise(stream_key, shape, scale, most, split, heavy, dtype=jnp.bfloat16):
    values = scale * jax.random.normal(stream_key, shape, jnp.float32)
    if split:
        values = values * shard_levels(stream_key, shape, split, -0.22, 0.18)
    return jnp.clip(with_spikes(values, jax.random.fold_in(stream_key, 3), *heavy), -most, most).astype(dtype)


def setup_inputs(seed: int = 0) -> dict:
    streams_of = jax.random.split(jax.random.key(seed), 8)
    return {
        "grads": heavy_noise(streams_of[0], (REPLICAS, TENSORS, D, KVW), 1.0, 6.0, ((0, 8), (3, 4)), (0, 2, 8, 2.0)),
        "param": gaussian(streams_of[1], (TENSORS, D, KVW), 0.5, 3.0, ((1, 8), (2, 4)), jnp.float32),
        "q_m": jnp.clip(jax.random.uniform(streams_of[2], (TENSORS, D, KVW), jnp.float32, -1.0, 1.0) * shard_levels(streams_of[2], (TENSORS, D, KVW), ((1, 8), (2, 4)), -0.4, 0.0), -1.0, 1.0).astype(jnp.bfloat16),
        "m_scale": jnp.clip(jnp.exp(jax.random.uniform(streams_of[3], (TENSORS,), jnp.float32, math.log(0.02), math.log(0.2))), 0.02, 0.2),
        "q_v": jnp.clip(jnp.exp(math.log(1.0) - 6.9083047 * jax.random.uniform(streams_of[4], (TENSORS, D, KVW), jnp.float32) ** shard_levels(streams_of[4], (TENSORS, D, KVW), ((1, 8), (2, 4)), -0.2, 0.2)), 0.0009994507, 1.0).astype(jnp.bfloat16),
        "v_max": jnp.clip(jnp.exp(math.log(0.05) - 2.3025851 * jax.random.uniform(streams_of[5], (TENSORS, GROUPS), jnp.float32) ** shard_levels(streams_of[5], (TENSORS, GROUPS), ((1, 4),), -0.2, 0.2)), 0.005, 0.05),
        "v_exp": jnp.clip(1.0 + 9.0 * jax.random.uniform(streams_of[6], (TENSORS, GROUPS), jnp.float32) ** shard_levels(streams_of[6], (TENSORS, GROUPS), ((1, 4),), -0.2, 0.2), 1.0, 10.0),
    }


def reference(grads, param, q_m, m_scale, q_v, v_max, v_exp):

    def add_one(index, total):
        return total + lax.dynamic_index_in_dim(grads, index, 0, keepdims=False).astype(jnp.float32)
    summed = lax.fori_loop(0, REPLICAS, add_one, jnp.zeros((TENSORS, D, KVW), jnp.float32))
    grad = (summed / REPLICAS).reshape(TENSORS, D, GROUPS, HEAD)
    m_old = m_scale[:, None, None, None] * q_m.astype(jnp.float32).reshape(TENSORS, D, GROUPS, HEAD)
    stored = q_v.astype(jnp.float32).reshape(TENSORS, D, GROUPS, HEAD)
    v_old = v_max[:, None, :, None] * jnp.exp(jnp.log(stored) / v_exp[:, None, :, None])
    m_new = 0.9 * m_old + 0.1 * grad
    v_new = 0.95 * v_old + 0.05 * grad * grad
    weights = param.reshape(TENSORS, D, GROUPS, HEAD)
    new_param = weights - 0.02 * (m_new / (jnp.sqrt(v_new) + 1e-08) + 0.1 * weights)
    new_m_scale = lax.optimization_barrier(jnp.max(jnp.abs(m_new), axis=(1, 2, 3))) + 1e-06
    new_v_max = lax.optimization_barrier(jnp.max(v_new, axis=(1, 3)))
    v_low = lax.optimization_barrier(jnp.min(v_new, axis=(1, 3)))
    new_v_exp = 12.343 / jnp.maximum(jnp.log(new_v_max / v_low), 1.0)
    new_q_m = (m_new / new_m_scale[:, None, None, None]).astype(jnp.bfloat16)
    new_q_v = jnp.exp(new_v_exp[:, None, :, None] * jnp.log(v_new / new_v_max[:, None, :, None])).astype(jnp.bfloat16)
    shape = (TENSORS, D, KVW)
    return (new_param.reshape(shape), new_q_m.reshape(shape), new_m_scale, new_q_v.reshape(shape), new_v_max, new_v_exp)
```

```python
import functools

import jax
import jax.numpy as jnp
from jax import lax
from jax.experimental import pallas as pl
from jax.experimental.pallas import tpu as pltpu
from jax.sharding import PartitionSpec as P

MESH = pl.DeviceIdType.MESH
STEP = 32
SPLIT = 1
SLOTS = 3
RING = 4
LEAD = 5
LAG_A = 4
LAG_B = 5
LAG_B_INNER = 9
LAG_UPDATE = 5
LAG_FINISH = 3
LAG_SCALE = 2


def kernel(n, peers, *refs):
    (grads, param, q_m, q_v, m_scale, v_max, v_exp,
     out_p, out_m, out_v, out_s,
     raw, y_cast, a_cast, y_in, z_in, s_out, s_in,
     par, qm, qv, m_new, v_new, stat, stat_in, peak, peak_in,
     raw_sem, in_sem, out_sem, y_send, y_recv, z_send, z_recv, s_send, s_recv,
     st_send, st_recv, pk_send, pk_recv) = refs
    count, _, rows, width = grads.shape
    groups = v_max.shape[1]
    lanes = width // groups
    nz = n // 2
    chunk = rows // (8 * SPLIT)
    step = min(STEP, chunk)
    wide = 7 * SPLIT
    tall = 4 * SPLIT
    sides = 2 * SPLIT
    period = wide * nz + sides
    me = lax.axis_index("dp")
    mt = lax.axis_index("tensor")
    y = lax.rem(me, 2)
    z = me // 2
    half = z // (nz // 2)
    zm = z + half * (nz - 1 - 2 * z)
    is_outer = zm == 0
    is_inner = zm == 1
    inner = 1 + half * (nz - 3)

    def is_end(d):
        return 1 - (lax.rem(d, nz - 1) + nz - 2) // (nz - 1)

    def n_b(d):
        return SPLIT * (7 - is_end(d))

    def n_a(d):
        return SPLIT * (1 + is_end(d))

    def order(i):
        low = jnp.minimum(zm, 1)
        d = nz - 1 + low - i
        d = d - low * jnp.where(d <= zm, 1, 0)
        d = jnp.where((i == 0) & (zm > 0), 0, d)
        d = jnp.where(i == nz - 1, zm, d)
        return d + half * (nz - 1 - 2 * d)

    def through(d):
        return nz - 2 + d - 2 * (1 - half)

    barrier = pltpu.get_barrier_semaphore()

    def raw_copy(t):
        return pltpu.make_async_copy(grads.at[t], raw.at[t], raw_sem.at[t])

    def in_copies(t):
        return [pltpu.make_async_copy(src.at[t], dst.at[t], in_sem.at[t, i])
                for i, (src, dst) in enumerate(((q_m, qm), (q_v, qv), (param, par)))]

    def out_copy(src, dst, t, i):
        return pltpu.make_async_copy(src.at[t], dst.at[t], out_sem.at[t, i])

    for t in range(count):
        raw_copy(t).start()
    for t in range(count):
        for c in in_copies(t):
            c.start()

    def greet(o, _):
        pl.semaphore_signal(barrier, inc=1, device_id={"dp": lax.rem(me + o, n)}, device_id_type=MESH)
        return 0
    lax.fori_loop(1, n, greet, 0)

    def greet_t(o, _):
        pl.semaphore_signal(barrier, inc=1, device_id={"tensor": lax.rem(mt + o, peers)}, device_id_type=MESH)
        return 0
    lax.fori_loop(1, peers, greet_t, 0)
    pl.semaphore_wait(barrier, n - 1 + peers - 1)

    def remote(src, dst, s_sem, r_sem, to):
        return pltpu.make_async_remote_copy(src_ref=src, dst_ref=dst, send_sem=s_sem, recv_sem=r_sem,
                                            device_id={"dp": to}, device_id_type=MESH)

    def loop(body):
        def one(i, _):
            body(pl.ds(pl.multiple_of(i * step, step), step))
            return 0
        lax.fori_loop(0, chunk // step, one, 0)

    def mine(t, d, side, c, at):
        first = pl.multiple_of(c * chunk + at.start, step)
        return raw[t, d * 2 + side, pl.ds(first, step), :].astype(jnp.float32)

    def y_copy(t, d, c, ring):
        s = lax.rem(t, SLOTS)
        return remote(y_cast.at[ring], y_in.at[s, d, c], y_send.at[ring], y_recv.at[s, d, c], z * 2 + 1 - y)

    def s_copy(t, c):
        s = lax.rem(t, SLOTS)
        h = lax.rem(t, 2)
        return remote(s_out.at[h, c], s_in.at[s, c], s_send.at[h, c], s_recv.at[s, c], z * 2 + 1 - y)

    def z_wait(t, where, c):
        s = lax.rem(t, SLOTS)
        remote(z_in.at[s, where, c], z_in.at[s, where, c], z_send.at[0, 0], z_recv.at[s, where, c], me).wait_recv()

    def landed(t, c):
        for k in range(nz - 2):
            if nz > 4:
                @pl.when((zm <= 1) | (z != k + 1))
                def _():
                    z_wait(t, k, c)
            else:
                z_wait(t, k, c)

    def gathered(t, c, at):
        s = lax.rem(t, SLOTS)
        total = None
        for k in range(nz - 2):
            part = z_in[s, k, c, at, :]
            if nz > 4:
                part = jnp.where((zm <= 1) | (z != k + 1), part, 0.0)
            total = part if total is None else total + part
        return total

    def z_go(t, src, d, c, sem):
        s = lax.rem(t, SLOTS)
        to = jnp.where(is_outer, inner, d)
        where = jnp.where(is_outer, jnp.where(d == inner, d - 1, through(d)), z - 1)
        remote(src, z_in.at[s, where, c], sem, z_recv.at[s, where, c], to * 2 + y).start()

    def z_sent(sem):
        remote(a_cast.at[0, 0], a_cast.at[0, 0], sem, z_recv.at[0, 0, 0], me).wait_send()

    def y_job(t, i, c, ring, full):
        d = order(i)

        @pl.when(full)
        def _():
            y_copy(t, d, c, ring).wait_send()

        def body(at):
            y_cast[ring, at, :] = mine(t, d, 1 - y, c, at)
        loop(body)
        y_copy(t, d, c, ring).start()

    def s_job(t, c):
        h = lax.rem(t, 2)

        @pl.when(t >= 2)
        def _():
            s_copy(t, c).wait_send()
        j = n_b(z) + (1 - y) * n_a(z) + c
        landed(t, j)

        def body(at):
            s_out[h, c, at, :] = gathered(t, j, at) + mine(t, z, 1 - y, n_b(z) + c, at)
        loop(body)
        s_copy(t, c).start()

    def a_job(t, i, j):
        s = lax.rem(t, SLOTS)
        d = order(i)
        side = j // n_a(d)
        c = n_b(d) + lax.rem(j, n_a(d))
        k = n_b(d) + j
        sem = z_send.at[i, wide + j]

        @pl.when(t > 0)
        def _():
            z_sent(sem)
        relay = is_inner & (i > 0)

        @pl.when(relay)
        def _():
            w = through(d)
            z_wait(t, w, k)

            def body(at):
                z_in[s, w, k, at, :] = z_in[s, w, k, at, :] + mine(t, d, side, c, at)
            loop(body)
            z_go(t, z_in.at[s, w, k], d, k, sem)

        @pl.when(jnp.logical_not(relay))
        def _():
            def body(at):
                a_cast[i, j, at, :] = mine(t, d, side, c, at)
            loop(body)
            z_go(t, a_cast.at[i, j], d, k, sem)

    def b_job(t, i, c):
        s = lax.rem(t, SLOTS)
        d = order(i)
        sem = z_send.at[i, c]

        @pl.when(t > 0)
        def _():
            z_sent(sem)
        y_copy(t, d, c, 0).wait_recv()
        relay = is_inner & (i > 0)

        @pl.when(relay)
        def _():
            w = through(d)
            z_wait(t, w, c)

            def body(at):
                z_in[s, w, c, at, :] = z_in[s, w, c, at, :] + (y_in[s, d, c, at, :] + mine(t, d, y, c, at))
            loop(body)
            z_go(t, z_in.at[s, w, c], d, c, sem)

        @pl.when(jnp.logical_not(relay))
        def _():
            def body(at):
                y_in[s, d, c, at, :] = y_in[s, d, c, at, :] + mine(t, d, y, c, at)
            loop(body)
            z_go(t, y_in.at[s, d, c], d, c, sem)

    def update(t, c, total):
        scale = m_scale[t]
        h = lax.rem(t, 2)

        def fold(x):
            return jnp.max(x.reshape(step // 8, 8, lanes), axis=0)

        def one(it, carry):
            at = pl.ds(pl.multiple_of(it * step, step), step)
            whole = total(at) * (1.0 / n)
            rows_i = pl.ds(pl.multiple_of(c * chunk + it * step, step), step)
            top_m, tops, lows = carry
            new_tops, new_lows = [], []
            for g in range(groups):
                cols = slice(g * lanes, (g + 1) * lanes)
                grad = whole[:, cols]
                m_old = scale * qm[t, rows_i, cols].astype(jnp.float32)
                stored = qv[t, rows_i, cols].astype(jnp.float32)
                inv = 1.0 / jnp.full((1, lanes), v_exp[t, g], jnp.float32)
                v_old = v_max[t, g] * jnp.exp(jnp.log(stored) * inv)
                m = 0.9 * m_old + 0.1 * grad
                v = 0.95 * v_old + 0.05 * grad * grad
                w = par[t, rows_i, cols]
                par[t, rows_i, cols] = w - 0.02 * (m / (jnp.sqrt(v) + 1e-08) + 0.1 * w)
                m_new[h, rows_i, cols] = m
                v_new[h, rows_i, cols] = v
                top_m = jnp.maximum(top_m, fold(jnp.abs(m)))
                new_tops.append(jnp.maximum(tops[g], fold(v)))
                new_lows.append(jnp.maximum(lows[g], fold(-v)))
            return top_m, tuple(new_tops), tuple(new_lows)
        least = jnp.full((8, lanes), -jnp.inf, jnp.float32)
        top_m, tops, lows = lax.fori_loop(0, chunk // step, one, (least, (least,) * groups, (least,) * groups))
        for row, value in enumerate((top_m,) + tops + lows):
            stat[t, row:row + 1, :] = jnp.maximum(stat[t, row:row + 1, :], jnp.max(value, axis=0, keepdims=True))

    def update_a(t, c):
        s = lax.rem(t, SLOTS)

        @pl.when(c == 0)
        def _():
            for copy in in_copies(t):
                copy.wait()
            stat[t] = jnp.full(stat.shape[1:], -jnp.inf, jnp.float32)
        j = n_b(z) + y * n_a(z) + c
        landed(t, j)
        s_copy(t, c).wait_recv()
        update(t, n_b(z) + c,
               lambda at: gathered(t, j, at) + mine(t, z, y, n_b(z) + c, at) + s_in[s, c, at, :])

    def update_b(t, c):
        s = lax.rem(t, SLOTS)
        y_copy(t, z, c, 0).wait_recv()
        landed(t, c)
        update(t, c, lambda at: gathered(t, c, at) + (y_in[s, z, c, at, :] + mine(t, z, y, c, at)))

    def stat_copy(t, o):
        return pltpu.make_async_remote_copy(
            src_ref=stat.at[t], dst_ref=stat_in.at[t, o], send_sem=st_send.at[t, o], recv_sem=st_recv.at[t, o],
            device_id={"dp": lax.rem(me + o, n)}, device_id_type=MESH)

    def peak_copy(t, o):
        return pltpu.make_async_remote_copy(
            src_ref=peak.at[t], dst_ref=peak_in.at[t, o], send_sem=pk_send.at[t, o], recv_sem=pk_recv.at[t, o],
            device_id={"tensor": lax.rem(mt + o, peers)}, device_id_type=MESH)

    def each(lo, hi, act):
        def one(o, _):
            act(o)
            return 0
        lax.fori_loop(lo, hi, one, 0)

    def share(t):
        out_copy(par, out_p, t, 0).start()
        each(1, n, lambda o: stat_copy(t, o).start())

    def all_rows(body):
        def one(i, _):
            body(pl.ds(pl.multiple_of(i * STEP, STEP), STEP))
            return 0
        lax.fori_loop(0, rows // STEP, one, 0)

    def finish(t):
        h = lax.rem(t, 2)
        each(1, n, lambda o: stat_copy(t, o).wait_recv())
        best = lax.fori_loop(1, n, lambda o, b: jnp.maximum(b, stat_in[t, o]), stat[t])
        best = jnp.broadcast_to(jnp.max(best, axis=1, keepdims=True), best.shape)
        peak[t] = best
        each(1, peers, lambda o: peak_copy(t, o).start())
        exps, invs = [], []
        for g in range(groups):
            top = best[1 + g:2 + g, :]
            low = -best[1 + groups + g:2 + groups + g, :]
            exps.append(12.343 / jnp.maximum(jnp.log(top / low), 1.0))
            invs.append(1.0 / top)
            out_s[t, 1 + g:2 + g, :] = top
            out_s[t, 1 + groups + g:2 + groups + g, :] = exps[g]

        def body(at):
            for g in range(groups):
                cols = slice(g * lanes, (g + 1) * lanes)
                value = jnp.exp(exps[g] * jnp.log(v_new[h, at, cols] * invs[g]))
                qv[t, at, cols] = value.astype(jnp.bfloat16)
        all_rows(body)
        out_copy(qv, out_v, t, 1).start()

    def scale(t):
        h = lax.rem(t, 2)
        each(1, peers, lambda o: peak_copy(t, o).wait_recv())
        whole = lax.fori_loop(1, peers, lambda o, b: jnp.maximum(b, peak_in[t, o]), peak[t])[0:1, :] + 1e-06
        out_s[t, 0:1, :] = whole
        inverse = 1.0 / whole

        def body(at):
            for g in range(groups):
                cols = slice(g * lanes, (g + 1) * lanes)
                qm[t, at, cols] = (m_new[h, at, cols] * inverse).astype(jnp.bfloat16)
        all_rows(body)
        out_copy(qm, out_m, t, 2).start()

    lag_a = jnp.where(is_inner, LAG_A, -LEAD)
    lag_b = jnp.where(is_inner, LAG_B_INNER, LAG_B)
    own = wide * (nz - 1) + sides

    def place(g, lag):
        g = g - lag
        ok = (g >= 0) & (g < count * period)
        g = jnp.clip(g, 0, count * period - 1)
        return ok, g // period, lax.rem(g, period)

    def one(it, sent):
        g = it - LEAD
        ok, t, p = place(g, -LEAD)

        @pl.when(ok & (p == 0))
        def _():
            raw_copy(t).wait()

        ok, t, p = place(g, lag_a)
        i, j = jnp.minimum(p // tall, nz - 2), lax.rem(p, tall)

        @pl.when(ok & (p < tall * (nz - 1)) & (j < 2 * n_a(order(i))))
        def _():
            a_job(t, i, j)

        ok, t, p = place(g, 0)
        tail = p >= own
        i = jnp.where(tail, nz - 1, p // wide)
        c = jnp.where(tail, p - own, lax.rem(p, wide))
        live = ok & (tail | (p < own - sides)) & (c < n_b(order(i)))

        @pl.when(live)
        def _():
            y_job(t, i, c, lax.rem(sent, RING), sent >= RING)
        sent = sent + jnp.where(live, 1, 0)
        c = p - (own - sides)

        @pl.when(ok & (c >= 0) & (c < n_a(z)) & (p < own))
        def _():
            s_job(t, c)

        ok, t, p = place(g, lag_b)
        i, c = p // wide, lax.rem(p, wide)

        @pl.when(ok & (p < own - sides) & (c < n_b(order(i))))
        def _():
            b_job(t, i, c)

        ok, t, p = place(g, LAG_UPDATE)
        c = p - (own - sides)

        @pl.when(ok & (c >= 0) & (c < n_a(z)) & (p < own))
        def _():
            update_a(t, c)
        c = p - own

        @pl.when(ok & (c >= 0) & (c < n_b(z)))
        def _():
            update_b(t, c)

        @pl.when(ok & (p == period - 1))
        def _():
            share(t)

        ok, t, p = place(g, LAG_UPDATE + LAG_FINISH)

        @pl.when(ok & (p == period - 1))
        def _():
            finish(t)

        ok, t, p = place(g, LAG_UPDATE + LAG_FINISH + LAG_SCALE)

        @pl.when(ok & (p == period - 1))
        def _():
            scale(t)
        return sent

    steps = LEAD + count * period + LAG_UPDATE + LAG_FINISH + LAG_SCALE
    lax.fori_loop(0, steps, one, 0)

    each(0, RING, lambda r: y_copy(0, 0, 0, r).wait_send())

    def drain(i, _):
        d = order(i)
        each(0, n_b(d), lambda c: z_sent(z_send.at[i, c]))
        each(0, 2 * n_a(d), lambda j: z_sent(z_send.at[i, wide + j]))
        return 0
    lax.fori_loop(0, nz - 1, drain, 0)
    for t in range(max(0, count - 2), count):
        each(0, n_a(z), lambda c: s_copy(t, c).wait_send())
    for t in range(count):
        each(1, n, lambda o: stat_copy(t, o).wait_send())
        each(1, peers, lambda o: peak_copy(t, o).wait_send())
        out_copy(par, out_p, t, 0).wait()
        out_copy(qv, out_v, t, 1).wait()
        out_copy(qm, out_m, t, 2).wait()


def on_device(n, peers, grads, param, q_m, m_scale, q_v, v_max, v_exp):
    count, rows, width = q_m.shape
    groups = v_max.shape[1]
    lanes = width // groups
    nz = n // 2
    chunk = rows // (8 * SPLIT)
    wide, tall, deep = 7 * SPLIT, 4 * SPLIT, 10 * SPLIT
    kinds = -(-(1 + 2 * groups) // 8) * 8
    f32, bf16 = jnp.float32, jnp.bfloat16
    dma = pltpu.SemaphoreType.DMA
    hbm = pl.BlockSpec(memory_space=pl.ANY)
    smem = pl.BlockSpec(memory_space=pltpu.SMEM)
    new_param, new_q_m, new_q_v, stats = pl.pallas_call(
        functools.partial(kernel, n, peers),
        out_shape=(
            jax.ShapeDtypeStruct(param.shape, f32),
            jax.ShapeDtypeStruct(q_m.shape, bf16),
            jax.ShapeDtypeStruct(q_v.shape, bf16),
            jax.ShapeDtypeStruct((count, kinds, lanes), f32),
        ),
        in_specs=[hbm] * 4 + [smem] * 3,
        out_specs=(hbm, hbm, hbm, pl.BlockSpec(memory_space=pltpu.VMEM)),
        scratch_shapes=[
            pltpu.VMEM((count, n, rows, width), bf16),
            pltpu.VMEM((RING, chunk, width), f32),
            pltpu.VMEM((nz - 1, tall, chunk, width), f32),
            pltpu.VMEM((SLOTS, nz, wide, chunk, width), f32),
            pltpu.VMEM((SLOTS, 2 * (nz - 2), deep, chunk, width), f32),
            pltpu.VMEM((2, 2 * SPLIT, chunk, width), f32),
            pltpu.VMEM((SLOTS, 2 * SPLIT, chunk, width), f32),
            pltpu.VMEM(param.shape, f32),
            pltpu.VMEM(q_m.shape, bf16),
            pltpu.VMEM(q_v.shape, bf16),
            pltpu.VMEM((2, rows, width), f32),
            pltpu.VMEM((2, rows, width), f32),
            pltpu.VMEM((count, kinds, lanes), f32),
            pltpu.VMEM((count, n, kinds, lanes), f32),
            pltpu.VMEM((count, kinds, lanes), f32),
            pltpu.VMEM((count, peers, kinds, lanes), f32),
            dma((count,)), dma((count, 3)), dma((count, 3)),
            dma((RING,)), dma((SLOTS, nz, wide)),
            dma((nz - 1, wide + tall)), dma((SLOTS, 2 * (nz - 2), deep)),
            dma((2, 2 * SPLIT)), dma((SLOTS, 2 * SPLIT)),
            dma((count, n)), dma((count, n)),
            dma((count, peers)), dma((count, peers)),
        ],
        compiler_params=pltpu.CompilerParams(
            collective_id=0, has_side_effects=True, vmem_limit_bytes=67043328
        ),
    )(grads[0].reshape(count, n, rows, width), param, q_m, q_v, m_scale, v_max, v_exp)
    new_m_scale = stats[:, 0, 0]
    group_top = stats[:, 1:1 + groups, 0]
    new_v_exp = stats[:, 1 + groups:1 + 2 * groups, 0]
    return new_param, new_q_m, new_m_scale, new_q_v, group_top, new_v_exp


def solution(mesh):
    in_specs = (
        P("dp", None, None, "tensor"),
        P(None, "dp", "tensor"),
        P(None, "dp", "tensor"),
        P(),
        P(None, "dp", "tensor"),
        P(None, "tensor"),
        P(None, "tensor"),
    )
    out_specs = (
        P(None, "dp", "tensor"),
        P(None, "dp", "tensor"),
        P(),
        P(None, "dp", "tensor"),
        P(None, "tensor"),
        P(None, "tensor"),
    )
    return jax.shard_map(
        functools.partial(on_device, mesh.shape["dp"], mesh.shape["tensor"]),
        mesh=mesh, in_specs=in_specs, out_specs=out_specs, check_vma=False
    )
```

```python
import functools
import math

import jax
import jax.numpy as jnp
from jax import lax
from jax.experimental import pallas as pl
from jax.experimental.pallas import tpu as pltpu
from jax.sharding import PartitionSpec as P

MESH = pl.DeviceIdType.MESH
STEP = 32
LONG = 128
SPLIT = 1
SLOTS = 3
RING = 4
Z_RING = 16
LEAD = 1
LAG_A = 4
LAG_B = 5
LAG_B_INNER = 9
LAG_UPDATE = 5
LAG_FINISH = 10
LAG_SCALE = 5
SPARE = 1 << 20


def kernel(n, peers, *refs):
    (grads, param, q_m, q_v, m_scale, v_max, v_exp,
     par, qm, qv, m_new, v_new, out_s,
     raw, y_cast, a_cast, y_in, z_in, s_out, s_in,
     stat, stat_in, peak, peak_in,
     raw_sem, in_sem, y_send, y_recv, z_send, z_recv, s_send, s_recv,
     st_send, st_recv, pk_send, pk_recv) = refs
    count, _, rows, width = grads.shape
    groups = v_max.shape[0]
    lanes = width // groups
    nz = n // 2
    chunk = rows // (8 * SPLIT)
    step = min(STEP, chunk)
    wide = 7 * SPLIT
    tall = 4 * SPLIT
    sides = 2 * SPLIT
    period = wide * nz + sides
    me = lax.axis_index("dp")
    mt = lax.axis_index("tensor")
    y = lax.rem(me, 2)
    z = me // 2
    half = z // (nz // 2)
    zm = z + half * (nz - 1 - 2 * z)
    is_outer = zm == 0
    is_inner = zm == 1
    inner = 1 + half * (nz - 3)

    def is_end(d):
        return 1 - (lax.rem(d, nz - 1) + nz - 2) // (nz - 1)

    def n_b(d):
        return SPLIT * (7 - is_end(d))

    def n_a(d):
        return SPLIT * (1 + is_end(d))

    def order(i):
        low = jnp.minimum(zm, 1)
        d = nz - 1 + low - i
        d = d - low * jnp.where(d <= zm, 1, 0)
        d = jnp.where((i == 0) & (zm > 0), 0, d)
        d = jnp.where(i == nz - 1, zm, d)
        return d + half * (nz - 1 - 2 * d)

    def through(d):
        return nz - 2 + d - 2 * (1 - half)

    barrier = pltpu.get_barrier_semaphore()

    raws = [pltpu.make_async_copy(grads.at[at], raw.at[at], raw_sem.at[i])
            for i, at in enumerate((pl.ds(0, 1), pl.ds(1, count - 1)))]
    ins = [pltpu.make_async_copy(src, dst, in_sem.at[i])
           for i, (src, dst) in enumerate(((q_m, qm), (q_v, qv), (param, par)))]
    for c in raws + ins:
        c.start()

    def greet(o, _):
        pl.semaphore_signal(barrier, inc=1, device_id={"dp": lax.rem(me + o, n)}, device_id_type=MESH)
        return 0
    lax.fori_loop(1, n, greet, 0)

    def greet_t(o, _):
        pl.semaphore_signal(barrier, inc=1, device_id={"tensor": lax.rem(mt + o, peers)}, device_id_type=MESH)
        return 0
    lax.fori_loop(1, peers, greet_t, 0)
    pl.semaphore_wait(barrier, n - 1 + peers - 1)

    def remote(src, dst, s_sem, r_sem, to):
        return pltpu.make_async_remote_copy(src_ref=src, dst_ref=dst, send_sem=s_sem, recv_sem=r_sem,
                                            device_id={"dp": to}, device_id_type=MESH)

    def loop(body):
        def one(i, _):
            body(pl.ds(pl.multiple_of(i * step, step), step))
            return 0
        lax.fori_loop(0, chunk // step, one, 0)

    def mine(t, d, side, c, at):
        first = pl.multiple_of(c * chunk + at.start, step)
        return raw[t, d * 2 + side, pl.ds(first, step), :].astype(jnp.float32)

    def y_copy(t, d, c, ring):
        s = lax.rem(t, SLOTS)
        return remote(y_cast.at[ring], y_in.at[s, d, c], y_send.at[ring], y_recv.at[d, c], z * 2 + 1 - y)

    def s_copy(t, c):
        s = lax.rem(t, SLOTS)
        return remote(s_out.at[c], s_in.at[s, c], s_send.at[c], s_recv.at[c], z * 2 + 1 - y)

    def z_wait(t, where, c):
        s = lax.rem(t, SLOTS)
        remote(z_in.at[s, where, c], z_in.at[s, where, c], z_send.at[0], z_recv.at[lax.rem(t, 2), where, c], me).wait_recv()

    def landed(t, c):
        for k in range(nz - 2):
            if nz > 4:
                @pl.when((zm <= 1) | (z != k + 1))
                def _():
                    z_wait(t, k, c)
            else:
                z_wait(t, k, c)

    def gathered(t, c, at):
        s = lax.rem(t, SLOTS)
        total = None
        for k in range(nz - 2):
            part = z_in[s, k, c, at, :]
            if nz > 4:
                part = jnp.where((zm <= 1) | (z != k + 1), part, 0.0)
            total = part if total is None else total + part
        return total

    def z_go(t, src, d, c, sem):
        s = lax.rem(t, SLOTS)
        to = jnp.where(is_outer, inner, d)
        where = jnp.where(is_outer, jnp.where(d == inner, d - 1, through(d)), z - 1)
        remote(src, z_in.at[s, where, c], sem, z_recv.at[lax.rem(t, 2), where, c], to * 2 + y).start()

    def z_sent(sem):
        remote(a_cast.at[0, 0], a_cast.at[0, 0], sem, z_recv.at[0, 0, 0], me).wait_send()

    def y_job(t, i, c, ring, full):
        d = order(i)

        @pl.when(full)
        def _():
            y_copy(t, d, c, ring).wait_send()

        def body(at):
            y_cast[ring, at, :] = mine(t, d, 1 - y, c, at)
        loop(body)
        y_copy(t, d, c, ring).start()

    def s_job(t, c):
        @pl.when(t > 0)
        def _():
            s_copy(t, c).wait_send()
        j = n_b(z) + (1 - y) * n_a(z) + c
        landed(t, j)

        def body(at):
            s_out[c, at, :] = gathered(t, j, at) + mine(t, z, 1 - y, n_b(z) + c, at)
        loop(body)
        s_copy(t, c).start()

    def a_job(t, i, j, gone):
        s = lax.rem(t, SLOTS)
        d = order(i)
        side = j // n_a(d)
        c = n_b(d) + lax.rem(j, n_a(d))
        k = n_b(d) + j
        sem = z_send.at[lax.rem(gone, Z_RING)]

        @pl.when(gone >= Z_RING)
        def _():
            z_sent(sem)
        relay = is_inner & (i > 0)

        @pl.when(relay)
        def _():
            w = through(d)
            z_wait(t, w, k)

            def body(at):
                z_in[s, w, k, at, :] = z_in[s, w, k, at, :] + mine(t, d, side, c, at)
            loop(body)
            z_go(t, z_in.at[s, w, k], d, k, sem)

        @pl.when(jnp.logical_not(relay))
        def _():
            def body(at):
                a_cast[i, j, at, :] = mine(t, d, side, c, at)
            loop(body)
            z_go(t, a_cast.at[i, j], d, k, sem)

    def b_job(t, i, c, gone):
        s = lax.rem(t, SLOTS)
        d = order(i)
        sem = z_send.at[lax.rem(gone, Z_RING)]

        @pl.when(gone >= Z_RING)
        def _():
            z_sent(sem)
        y_copy(t, d, c, 0).wait_recv()
        relay = is_inner & (i > 0)

        @pl.when(relay)
        def _():
            w = through(d)
            z_wait(t, w, c)

            def body(at):
                z_in[s, w, c, at, :] = z_in[s, w, c, at, :] + (y_in[s, d, c, at, :] + mine(t, d, y, c, at))
            loop(body)
            z_go(t, z_in.at[s, w, c], d, c, sem)

        @pl.when(jnp.logical_not(relay))
        def _():
            def body(at):
                y_in[s, d, c, at, :] = y_in[s, d, c, at, :] + mine(t, d, y, c, at)
            loop(body)
            z_go(t, y_in.at[s, d, c], d, c, sem)

    def update(t, c, total):
        scale = m_scale[t]
        h = lax.rem(t, 2)

        def fold(x):
            return jnp.max(x.reshape(step // 8, 8, lanes), axis=0)

        def one(it, carry):
            at = pl.ds(pl.multiple_of(it * step, step), step)
            whole = total(at) * (1.0 / n)
            rows_i = pl.ds(pl.multiple_of(c * chunk + it * step, step), step)
            top_m, tops, lows = carry
            new_tops, new_lows = [], []
            for g in range(groups):
                cols = slice(g * lanes, (g + 1) * lanes)
                grad = whole[:, cols]
                m_old = scale * qm[t, rows_i, cols].astype(jnp.float32)
                stored = qv[t, rows_i, cols].astype(jnp.float32)
                inv = 1.0 / jnp.full((1, lanes), v_exp[g, t], jnp.float32)
                v_old = v_max[g, t] * jnp.exp(jnp.log(stored) * inv)
                m = 0.9 * m_old + 0.1 * grad
                v = 0.95 * v_old + 0.05 * grad * grad
                w = par[t, rows_i, cols]
                par[t, rows_i, cols] = w - 0.02 * (m / (jnp.sqrt(v) + 1e-08) + 0.1 * w)
                m_new[h, rows_i, cols] = m
                v_new[h, rows_i, cols] = v
                top_m = jnp.maximum(top_m, fold(jnp.abs(m)))
                new_tops.append(jnp.maximum(tops[g], fold(v)))
                new_lows.append(jnp.maximum(lows[g], fold(-v)))
            return top_m, tuple(new_tops), tuple(new_lows)
        least = jnp.full((8, lanes), -jnp.inf, jnp.float32)
        top_m, tops, lows = lax.fori_loop(0, chunk // step, one, (least, (least,) * groups, (least,) * groups))
        for row, value in enumerate((top_m,) + tops + lows):
            stat[t, row:row + 1, :] = jnp.maximum(stat[t, row:row + 1, :], jnp.max(value, axis=0, keepdims=True))

    def update_a(t, c):
        s = lax.rem(t, SLOTS)

        @pl.when((c == 0) & (t == 0))
        def _():
            for copy in ins:
                copy.wait()

        @pl.when(c == 0)
        def _():
            stat[t] = jnp.full(stat.shape[1:], -jnp.inf, jnp.float32)
        j = n_b(z) + y * n_a(z) + c
        landed(t, j)
        s_copy(t, c).wait_recv()
        update(t, n_b(z) + c,
               lambda at: gathered(t, j, at) + mine(t, z, y, n_b(z) + c, at) + s_in[s, c, at, :])

    def update_b(t, c):
        s = lax.rem(t, SLOTS)
        y_copy(t, z, c, 0).wait_recv()
        landed(t, c)
        update(t, c, lambda at: gathered(t, c, at) + (y_in[s, z, c, at, :] + mine(t, z, y, c, at)))

    def stat_copy(t, o):
        h = lax.rem(t, 2)
        return pltpu.make_async_remote_copy(
            src_ref=stat.at[t], dst_ref=stat_in.at[h, o], send_sem=st_send.at[h], recv_sem=st_recv.at[h],
            device_id={"dp": lax.rem(me + o, n)}, device_id_type=MESH)

    def peak_copy(t, o):
        h = lax.rem(t, 2)
        return pltpu.make_async_remote_copy(
            src_ref=peak.at[t], dst_ref=peak_in.at[h, o], send_sem=pk_send.at[h], recv_sem=pk_recv.at[h],
            device_id={"tensor": lax.rem(mt + o, peers)}, device_id_type=MESH)

    def stats_of(t):
        h = lax.rem(t, 2)
        return remote(stat_in.at[h, pl.ds(1, n - 1)], stat_in.at[h, pl.ds(1, n - 1)], st_send.at[h], st_recv.at[h], me)

    def peaks_of(t):
        h = lax.rem(t, 2)
        return remote(peak_in.at[h, pl.ds(1, peers - 1)], peak_in.at[h, pl.ds(1, peers - 1)],
                      pk_send.at[h], pk_recv.at[h], me)

    def each(lo, hi, act):
        def one(o, _):
            act(o)
            return 0
        lax.fori_loop(lo, hi, one, 0)

    def share(t):
        if isinstance(t, int):
            if t >= 2:
                stats_of(t).wait_send()
        else:
            @pl.when(t >= 2)
            def _():
                stats_of(t).wait_send()
        each(1, n, lambda o: stat_copy(t, o).start())

    def all_rows(body):
        def one(i, _):
            body(pl.ds(pl.multiple_of(i * LONG, LONG), LONG))
            return 0
        lax.fori_loop(0, rows // LONG, one, 0)

    def finish(t):
        h = lax.rem(t, 2)
        stats_of(t).wait_recv()
        best = lax.fori_loop(1, n, lambda o, b: jnp.maximum(b, stat_in[h, o]), stat[t])
        best = jnp.broadcast_to(jnp.max(best, axis=1, keepdims=True), best.shape)
        peak[t] = best
        if isinstance(t, int):
            if t >= 2:
                peaks_of(t).wait_send()
        else:
            @pl.when(t >= 2)
            def _():
                peaks_of(t).wait_send()
        each(1, peers, lambda o: peak_copy(t, o).start())
        exps, invs = [], []
        for g in range(groups):
            top = best[1 + g:2 + g, :]
            low = -best[1 + groups + g:2 + groups + g, :]
            exps.append(12.343 / jnp.maximum(jnp.log(top / low), 1.0))
            invs.append(1.0 / top)
            out_s[t, 1 + g:2 + g, :] = top
            out_s[t, 1 + groups + g:2 + groups + g, :] = exps[g]

        def body(at):
            for g in range(groups):
                cols = slice(g * lanes, (g + 1) * lanes)
                value = jnp.exp(exps[g] * jnp.log(v_new[h, at, cols] * invs[g]))
                qv[t, at, cols] = value.astype(jnp.bfloat16)
        if not isinstance(t, int):
            all_rows(body)

    def scale(t):
        h = lax.rem(t, 2)
        peaks_of(t).wait_recv()
        whole = lax.fori_loop(1, peers, lambda o, b: jnp.maximum(b, peak_in[h, o]), peak[t])[0:1, :] + 1e-06
        out_s[t, 0:1, :] = whole
        inverse = 1.0 / whole

        def body(at):
            for g in range(groups):
                cols = slice(g * lanes, (g + 1) * lanes)
                qm[t, at, cols] = (m_new[h, at, cols] * inverse).astype(jnp.bfloat16)
        if not isinstance(t, int):
            all_rows(body)

    lag_a = jnp.where(is_inner, LAG_A, -LEAD)
    lag_b = jnp.where(is_inner, LAG_B_INNER, LAG_B)
    own = wide * (nz - 1) + sides

    def place(g, lag):
        g = g - lag
        ok = (g >= 0) & (g < count * period)
        g = jnp.clip(g, 0, count * period - 1)
        return ok, g // period, lax.rem(g, period)

    def one(it, carry):
        sent, gone = carry
        g = it - LEAD
        ok, t, p = place(g, -LEAD)

        for u, c in enumerate(raws):
            @pl.when(ok & (p == 0) & (t == u))
            def _():
                c.wait()

        ok, t, p = place(g, lag_a)
        i, j = jnp.minimum(p // tall, nz - 2), lax.rem(p, tall)

        live = ok & (p < tall * (nz - 1)) & (j < 2 * n_a(order(i)))

        @pl.when(live)
        def _():
            a_job(t, i, j, gone)
        gone = gone + jnp.where(live, 1, 0)

        ok, t, p = place(g, 0)
        tail = p >= own
        i = jnp.where(tail, nz - 1, p // wide)
        c = jnp.where(tail, p - own, lax.rem(p, wide))
        live = ok & (tail | (p < own - sides)) & (c < n_b(order(i)))

        @pl.when(live)
        def _():
            y_job(t, i, c, lax.rem(sent, RING), sent >= RING)
        sent = sent + jnp.where(live, 1, 0)
        c = p - (own - sides)

        @pl.when(ok & (c >= 0) & (c < n_a(z)) & (p < own))
        def _():
            s_job(t, c)

        ok, t, p = place(g, lag_b)
        i, c = p // wide, lax.rem(p, wide)

        live = ok & (p < own - sides) & (c < n_b(order(i)))

        @pl.when(live)
        def _():
            b_job(t, i, c, gone)
        gone = gone + jnp.where(live, 1, 0)

        ok, t, p = place(g, LAG_UPDATE)
        c = p - (own - sides)

        @pl.when(ok & (c >= 0) & (c < n_a(z)) & (p < own))
        def _():
            update_a(t, c)
        c = p - own

        @pl.when(ok & (c >= 0) & (c < n_b(z)))
        def _():
            update_b(t, c)

        @pl.when(ok & (p == period - 1) & (t < count - 1))
        def _():
            share(t)

        ok, t, p = place(g, LAG_UPDATE + LAG_FINISH)

        @pl.when(ok & (p == period - 1))
        def _():
            finish(t)

        ok, t, p = place(g, LAG_UPDATE + LAG_FINISH + LAG_SCALE)

        @pl.when(ok & (p == period - 1))
        def _():
            scale(t)
        return sent, gone

    lax.fori_loop(0, LEAD + count * period + LAG_UPDATE, one, (0, 0))
    share(count - 1)
    finish(count - 1)
    scale(count - 1)

    each(0, RING, lambda r: y_copy(0, 0, 0, r).wait_send())

    each(0, Z_RING, lambda r: z_sent(z_send.at[r]))
    each(0, n_a(z), lambda c: s_copy(0, c).wait_send())
    for t in range(max(0, count - 2), count):
        stats_of(t).wait_send()
        peaks_of(t).wait_send()


def last(par, qm, qv, m_new, v_new, stats, out_p, out_m, out_v, out_scale, out_top, out_exp,
         qm_last, qv_last, sem):
    count, rows, width = par.shape
    groups = out_top.shape[0]
    lanes = width // groups
    t = count - 1
    h = t % 2
    copies = [pltpu.make_async_copy(par, out_p, sem.at[0])]
    for i, (src, dst) in enumerate(((qm, out_m), (qv, out_v))):
        if count > 1:
            copies.append(pltpu.make_async_copy(src.at[pl.ds(0, t)], dst.at[pl.ds(0, t)], sem.at[1 + i]))
    for c in copies:
        c.start()
    lane = lax.broadcasted_iota(jnp.int32, (1, lanes), 1)

    def packed(row):
        line = stats[0, row:row + 1, :]
        for u in range(1, count):
            line = jnp.where(lane == u, stats[u, row:row + 1, :], line)
        return line[:, :count]
    out_scale[...] = packed(0)
    for g in range(groups):
        out_top[g:g + 1, :] = packed(1 + g)
        out_exp[g:g + 1, :] = packed(1 + groups + g)
    inverse = 1.0 / stats[t, 0:1, :]
    invs = [1.0 / stats[t, 1 + g:2 + g, :] for g in range(groups)]
    exps = [stats[t, 1 + groups + g:2 + groups + g, :] for g in range(groups)]

    def body(i, _):
        at = pl.ds(pl.multiple_of(i * LONG, LONG), LONG)
        for g in range(groups):
            cols = slice(g * lanes, (g + 1) * lanes)
            value = jnp.exp(exps[g] * jnp.log(v_new[h, at, cols] * invs[g]))
            qv_last[at, cols] = value.astype(jnp.bfloat16)
            qm_last[at, cols] = (m_new[h, at, cols] * inverse).astype(jnp.bfloat16)
        return 0
    lax.fori_loop(0, rows // LONG, body, 0)
    for i, (src, dst) in enumerate(((qm_last, out_m), (qv_last, out_v))):
        c = pltpu.make_async_copy(src, dst.at[t], sem.at[3 + i])
        c.start()
        copies.append(c)
    for c in copies:
        c.wait()


def on_device(n, peers, grads, param, q_m, m_scale, q_v, v_max, v_exp):
    count, rows, width = q_m.shape
    groups = v_max.shape[1]
    lanes = width // groups
    nz = n // 2
    chunk = rows // (8 * SPLIT)
    wide, tall, deep = 7 * SPLIT, 4 * SPLIT, 10 * SPLIT
    kinds = -(-(1 + 2 * groups) // 8) * 8
    f32, bf16 = jnp.float32, jnp.bfloat16
    dma = pltpu.SemaphoreType.DMA
    hbm = pl.BlockSpec(memory_space=pl.ANY)
    smem = pl.BlockSpec(memory_space=pltpu.SMEM)
    vmem = pl.BlockSpec(memory_space=pltpu.VMEM)
    buffers = [
        pltpu.VMEM((count, n, rows, width), bf16),
        pltpu.VMEM((RING, chunk, width), f32),
        pltpu.VMEM((nz - 1, tall, chunk, width), f32),
        pltpu.VMEM((SLOTS, nz, wide, chunk, width), f32),
        pltpu.VMEM((SLOTS, 2 * (nz - 2), deep, chunk, width), f32),
        pltpu.VMEM((2 * SPLIT, chunk, width), f32),
        pltpu.VMEM((SLOTS, 2 * SPLIT, chunk, width), f32),
        pltpu.VMEM((count, kinds, lanes), f32),
        pltpu.VMEM((2, n, kinds, lanes), f32),
        pltpu.VMEM((count, kinds, lanes), f32),
        pltpu.VMEM((2, peers, kinds, lanes), f32),
    ]
    grant = SPARE + sum(math.prod(b.shape) * b.dtype.itemsize for b in buffers)
    state = pl.pallas_call(
        functools.partial(kernel, n, peers),
        out_shape=(
            pltpu.VMEM(param.shape, f32),
            pltpu.VMEM(q_m.shape, bf16),
            pltpu.VMEM(q_v.shape, bf16),
            pltpu.VMEM((2, rows, width), f32),
            pltpu.VMEM((2, rows, width), f32),
            pltpu.VMEM((count, kinds, lanes), f32),
        ),
        in_specs=[hbm] * 4 + [smem] * 3,
        out_specs=[vmem] * 6,
        scratch_shapes=buffers + [
            dma((2,)), dma((3,)),
            dma((RING,)), dma((nz, wide)),
            dma((Z_RING,)), dma((2, 2 * (nz - 2), deep)),
            dma((2 * SPLIT,)), dma((2 * SPLIT,)),
            dma((2,)), dma((2,)), dma((2,)), dma((2,)),
        ],
        compiler_params=pltpu.CompilerParams(
            collective_id=0, has_side_effects=True, vmem_limit_bytes=grant
        ),
    )(grads[0].reshape(count, n, rows, width), param, q_m, q_v, m_scale, v_max.T, v_exp.T)
    new_param, new_q_m, new_q_v, scales, tops, exps = pl.pallas_call(
        last,
        out_shape=(
            jax.ShapeDtypeStruct(param.shape, f32),
            jax.ShapeDtypeStruct(q_m.shape, bf16),
            jax.ShapeDtypeStruct(q_v.shape, bf16),
            jax.ShapeDtypeStruct((1, count), f32),
            jax.ShapeDtypeStruct((groups, count), f32),
            jax.ShapeDtypeStruct((groups, count), f32),
        ),
        in_specs=[vmem] * 6,
        out_specs=[hbm] * 3 + [vmem] * 3,
        scratch_shapes=[
            pltpu.VMEM((rows, width), bf16),
            pltpu.VMEM((rows, width), bf16),
            dma((5,)),
        ],
        compiler_params=pltpu.CompilerParams(vmem_limit_bytes=4 << 20),
    )(*state)
    return new_param, new_q_m, scales.reshape(count), new_q_v, tops.T, exps.T


def solution(mesh):
    in_specs = (
        P("dp", None, None, "tensor"),
        P(None, "dp", "tensor"),
        P(None, "dp", "tensor"),
        P(),
        P(None, "dp", "tensor"),
        P(None, "tensor"),
        P(None, "tensor"),
    )
    out_specs = (
        P(None, "dp", "tensor"),
        P(None, "dp", "tensor"),
        P(),
        P(None, "dp", "tensor"),
        P(None, "tensor"),
        P(None, "tensor"),
    )
    return jax.shard_map(
        functools.partial(on_device, mesh.shape["dp"], mesh.shape["tensor"]),
        mesh=mesh, in_specs=in_specs, out_specs=out_specs, check_vma=False
    )
```

```python
import functools
import math

import jax
import jax.numpy as jnp
from jax import lax
from jax.experimental import pallas as pl
from jax.experimental.pallas import tpu as pltpu
from jax.sharding import PartitionSpec as P

MESH = pl.DeviceIdType.MESH
STEP = 32
LONG = 128
SPLIT = 1
SLOTS = 3
RING = 4
Z_RING = 16
LEAD = 1
LAG_A = 4
LAG_B = 5
LAG_B_INNER = 9
LAG_UPDATE = 5
LAG_FINISH = 10
SPARE = 1 << 20


def merged(n, groups, row, row_in, out, t, h):
    lane = lax.broadcasted_iota(jnp.int32, row.shape[1:], 1)

    def pick(line, k):
        return jnp.broadcast_to(jnp.max(jnp.where(lane == k, line, -jnp.inf), axis=1, keepdims=True), line.shape)
    best = jnp.maximum(row[h], jnp.max(row_in[h, pl.ds(1, n - 1)], axis=0))
    every = jnp.maximum(best, jnp.max(row_in[h, pl.ds(n, row_in.shape[1] - n)], axis=0))
    whole = pick(every, 0) + 1e-06
    out[t, 0:1, :] = whole
    exps, invs = [], []
    for g in range(groups):
        top = pick(best, 1 + g)
        low = -pick(best, 1 + groups + g)
        exps.append(12.343 / jnp.maximum(jnp.log(top / low), 1.0))
        invs.append(1.0 / top)
        out[t, 1 + g:2 + g, :] = top
        out[t, 1 + groups + g:2 + groups + g, :] = exps[g]
    return 1.0 / whole, exps, invs


def kernel(n, peers, *refs):
    (grads, param, q_m, q_v, m_scale, v_max, v_exp,
     par, qm, qv, m_new, v_new, out_s, row, row_in,
     raw, y_cast, a_cast, y_in, z_in, s_out, s_in,
     stat,
     first_sem, rest_sem, y_send, y_recv, z_send, z_recv, s_send, s_recv,
     st_send, st_recv) = refs
    count, _, rows, width = grads.shape
    groups = v_max.shape[0]
    lanes = width // groups
    nz = n // 2
    chunk = rows // (8 * SPLIT)
    step = min(STEP, chunk)
    wide = 7 * SPLIT
    tall = 4 * SPLIT
    sides = 2 * SPLIT
    period = wide * nz + sides
    me = lax.axis_index("dp")
    mt = lax.axis_index("tensor")
    y = lax.rem(me, 2)
    z = me // 2
    half = z // (nz // 2)
    zm = z + half * (nz - 1 - 2 * z)
    is_outer = zm == 0
    is_inner = zm == 1
    inner = 1 + half * (nz - 3)

    def is_end(d):
        return 1 - (lax.rem(d, nz - 1) + nz - 2) // (nz - 1)

    def n_b(d):
        return SPLIT * (7 - is_end(d))

    def n_a(d):
        return SPLIT * (1 + is_end(d))

    def order(i):
        low = jnp.minimum(zm, 1)
        d = nz - 1 + low - i
        d = d - low * jnp.where(d <= zm, 1, 0)
        d = jnp.where((i == 0) & (zm > 0), 0, d)
        d = jnp.where(i == nz - 1, zm, d)
        return d + half * (nz - 1 - 2 * d)

    def through(d):
        return nz - 2 + d - 2 * (1 - half)

    barrier = pltpu.get_barrier_semaphore()

    def first_copy(i):
        at = pl.ds(order(i) * 2, 2)
        return pltpu.make_async_copy(grads.at[0, at], raw.at[0, at], first_sem.at[i])

    later = pl.ds(1, count - 1)
    rest = [pltpu.make_async_copy(src, dst, rest_sem.at[i]) for i, (src, dst) in enumerate((
        (grads.at[later], raw.at[later]), (q_m, qm), (q_v, qv), (param, par)))]
    first_copy(0).start()

    def each(lo, hi, act):
        def one(o, _):
            act(o)
            return 0
        lax.fori_loop(lo, hi, one, 0)

    def greet(axis, to):
        pl.semaphore_signal(barrier, inc=1, device_id={axis: to}, device_id_type=MESH)

    def greet_z(o):
        @pl.when(jnp.logical_not(is_outer & ((z + o == nz - 1) | (z + o == nz))))
        def _():
            greet("dp", lax.rem(z + o, nz) * 2 + y)
    greet("dp", z * 2 + 1 - y)
    each(1, nz, greet_z)
    each(1, peers, lambda o: greet("tensor", lax.rem(mt + o, peers)))
    each(1, nz, lambda i: first_copy(i).start())
    pl.semaphore_wait(barrier, nz - 1 + jnp.minimum(zm, 1) + peers - 1)

    def remote(src, dst, s_sem, r_sem, to):
        return pltpu.make_async_remote_copy(src_ref=src, dst_ref=dst, send_sem=s_sem, recv_sem=r_sem,
                                            device_id={"dp": to}, device_id_type=MESH)

    def loop(body):
        def one(i, _):
            body(pl.ds(pl.multiple_of(i * step, step), step))
            return 0
        lax.fori_loop(0, chunk // step, one, 0)

    def mine(t, d, side, c, at):
        first = pl.multiple_of(c * chunk + at.start, step)
        return raw[t, d * 2 + side, pl.ds(first, step), :].astype(jnp.float32)

    def y_copy(t, d, c, ring):
        s = lax.rem(t, SLOTS)
        return remote(y_cast.at[ring], y_in.at[s, d, c], y_send.at[ring], y_recv.at[d, c], z * 2 + 1 - y)

    def s_copy(t, c):
        s = lax.rem(t, SLOTS)
        return remote(s_out.at[c], s_in.at[s, c], s_send.at[c], s_recv.at[c], z * 2 + 1 - y)

    def z_wait(t, where, c):
        s = lax.rem(t, SLOTS)
        remote(z_in.at[s, where, c], z_in.at[s, where, c], z_send.at[0], z_recv.at[lax.rem(t, 2), where, c], me).wait_recv()

    def landed(t, c):
        for k in range(nz - 2):
            if nz > 4:
                @pl.when((zm <= 1) | (z != k + 1))
                def _():
                    z_wait(t, k, c)
            else:
                z_wait(t, k, c)

    def gathered(t, c, at):
        s = lax.rem(t, SLOTS)
        total = None
        for k in range(nz - 2):
            part = z_in[s, k, c, at, :]
            if nz > 4:
                part = jnp.where((zm <= 1) | (z != k + 1), part, 0.0)
            total = part if total is None else total + part
        return total

    def z_go(t, src, d, c, sem):
        s = lax.rem(t, SLOTS)
        to = jnp.where(is_outer, inner, d)
        where = jnp.where(is_outer, jnp.where(d == inner, d - 1, through(d)), z - 1)
        remote(src, z_in.at[s, where, c], sem, z_recv.at[lax.rem(t, 2), where, c], to * 2 + y).start()

    def z_sent(sem):
        remote(a_cast.at[0, 0], a_cast.at[0, 0], sem, z_recv.at[0, 0, 0], me).wait_send()

    def y_job(t, i, c, ring, full):
        d = order(i)

        @pl.when(full)
        def _():
            y_copy(t, d, c, ring).wait_send()

        def body(at):
            y_cast[ring, at, :] = mine(t, d, 1 - y, c, at)
        loop(body)
        y_copy(t, d, c, ring).start()

    def s_job(t, c):
        @pl.when(t > 0)
        def _():
            s_copy(t, c).wait_send()
        j = n_b(z) + (1 - y) * n_a(z) + c
        landed(t, j)

        def body(at):
            s_out[c, at, :] = gathered(t, j, at) + mine(t, z, 1 - y, n_b(z) + c, at)
        loop(body)
        s_copy(t, c).start()

    def a_job(t, i, j, gone):
        s = lax.rem(t, SLOTS)
        d = order(i)
        side = j // n_a(d)
        c = n_b(d) + lax.rem(j, n_a(d))
        k = n_b(d) + j
        sem = z_send.at[lax.rem(gone, Z_RING)]

        @pl.when(gone >= Z_RING)
        def _():
            z_sent(sem)
        relay = is_inner & (i > 0)

        @pl.when(relay)
        def _():
            w = through(d)
            z_wait(t, w, k)

            def body(at):
                z_in[s, w, k, at, :] = z_in[s, w, k, at, :] + mine(t, d, side, c, at)
            loop(body)
            z_go(t, z_in.at[s, w, k], d, k, sem)

        @pl.when(jnp.logical_not(relay))
        def _():
            def body(at):
                a_cast[i, j, at, :] = mine(t, d, side, c, at)
            loop(body)
            z_go(t, a_cast.at[i, j], d, k, sem)

    def b_job(t, i, c, gone):
        s = lax.rem(t, SLOTS)
        d = order(i)
        sem = z_send.at[lax.rem(gone, Z_RING)]

        @pl.when(gone >= Z_RING)
        def _():
            z_sent(sem)
        y_copy(t, d, c, 0).wait_recv()
        relay = is_inner & (i > 0)

        @pl.when(relay)
        def _():
            w = through(d)
            z_wait(t, w, c)

            def body(at):
                z_in[s, w, c, at, :] = z_in[s, w, c, at, :] + (y_in[s, d, c, at, :] + mine(t, d, y, c, at))
            loop(body)
            z_go(t, z_in.at[s, w, c], d, c, sem)

        @pl.when(jnp.logical_not(relay))
        def _():
            def body(at):
                y_in[s, d, c, at, :] = y_in[s, d, c, at, :] + mine(t, d, y, c, at)
            loop(body)
            z_go(t, y_in.at[s, d, c], d, c, sem)

    def update(t, c, total):
        scale = m_scale[t]
        h = lax.rem(t, 2)

        def fold(x):
            return jnp.max(x.reshape(step // 8, 8, lanes), axis=0)

        def one(it, carry):
            at = pl.ds(pl.multiple_of(it * step, step), step)
            whole = total(at) * (1.0 / n)
            rows_i = pl.ds(pl.multiple_of(c * chunk + it * step, step), step)
            top_m, tops, lows = carry
            new_tops, new_lows = [], []
            for g in range(groups):
                cols = slice(g * lanes, (g + 1) * lanes)
                grad = whole[:, cols]
                m_old = scale * qm[t, rows_i, cols].astype(jnp.float32)
                stored = qv[t, rows_i, cols].astype(jnp.float32)
                inv = 1.0 / jnp.full((1, lanes), v_exp[g, t], jnp.float32)
                v_old = v_max[g, t] * jnp.exp(jnp.log(stored) * inv)
                m = 0.9 * m_old + 0.1 * grad
                v = 0.95 * v_old + 0.05 * grad * grad
                w = par[t, rows_i, cols]
                par[t, rows_i, cols] = w - 0.02 * (m / (jnp.sqrt(v) + 1e-08) + 0.1 * w)
                m_new[h, rows_i, cols] = m
                v_new[h, rows_i, cols] = v
                top_m = jnp.maximum(top_m, fold(jnp.abs(m)))
                new_tops.append(jnp.maximum(tops[g], fold(v)))
                new_lows.append(jnp.maximum(lows[g], fold(-v)))
            return top_m, tuple(new_tops), tuple(new_lows)
        least = jnp.full((8, lanes), -jnp.inf, jnp.float32)
        top_m, tops, lows = lax.fori_loop(0, chunk // step, one, (least, (least,) * groups, (least,) * groups))
        for row, value in enumerate((top_m,) + tops + lows):
            stat[t, row:row + 1, :] = jnp.maximum(stat[t, row:row + 1, :], jnp.max(value, axis=0, keepdims=True))

    def update_a(t, c):
        s = lax.rem(t, SLOTS)

        @pl.when((c == 0) & (t == 0))
        def _():
            for copy in rest[1:]:
                copy.wait()

        @pl.when(c == 0)
        def _():
            stat[t] = jnp.full(stat.shape[1:], -jnp.inf, jnp.float32)
        j = n_b(z) + y * n_a(z) + c
        landed(t, j)
        s_copy(t, c).wait_recv()
        update(t, n_b(z) + c,
               lambda at: gathered(t, j, at) + mine(t, z, y, n_b(z) + c, at) + s_in[s, c, at, :])

    def update_b(t, c):
        s = lax.rem(t, SLOTS)
        y_copy(t, z, c, 0).wait_recv()
        landed(t, c)
        update(t, c, lambda at: gathered(t, c, at) + (y_in[s, z, c, at, :] + mine(t, z, y, c, at)))

    def row_copy(t, o):
        h = lax.rem(t, 2)
        return pltpu.make_async_remote_copy(
            src_ref=row.at[h], dst_ref=row_in.at[h, o], send_sem=st_send.at[h], recv_sem=st_recv.at[h],
            device_id={"tensor": lax.rem(mt + o // n, peers), "dp": lax.rem(me + lax.rem(o, n), n)},
            device_id_type=MESH)

    def rows_of(t):
        h = lax.rem(t, 2)
        part = row_in.at[h, pl.ds(1, n * peers - 1)]
        return remote(part, part, st_send.at[h], st_recv.at[h], me)

    kinds = stat.shape[1]

    def share(t):
        h = lax.rem(t, 2)
        if not isinstance(t, int) or t >= 2:
            @pl.when(t >= 2)
            def _():
                rows_of(t).wait_send()
        best = jnp.broadcast_to(jnp.max(stat[t], axis=1, keepdims=True), (kinds, lanes))
        at = [lax.broadcasted_iota(jnp.int32, (kinds, lanes), i) for i in range(2)]
        row[h] = jnp.max(jnp.where(at[0] == at[1], best, -jnp.inf), axis=0, keepdims=True)
        each(1, n * peers, lambda o: row_copy(t, o).start())

    def all_rows(body):
        def one(i, _):
            body(pl.ds(pl.multiple_of(i * LONG, LONG), LONG))
            return 0
        lax.fori_loop(0, rows // LONG, one, 0)

    def finish(t):
        h = lax.rem(t, 2)
        rows_of(t).wait_recv()
        inverse, exps, invs = merged(n, groups, row, row_in, out_s, t, h)

        def body(at):
            for g in range(groups):
                cols = slice(g * lanes, (g + 1) * lanes)
                value = jnp.exp(exps[g] * jnp.log(v_new[h, at, cols] * invs[g]))
                qv[t, at, cols] = value.astype(jnp.bfloat16)
                qm[t, at, cols] = (m_new[h, at, cols] * inverse).astype(jnp.bfloat16)
        all_rows(body)

    lag_a = jnp.where(is_inner, LAG_A, -LEAD)
    lag_b = jnp.where(is_inner, LAG_B_INNER, LAG_B)
    own = wide * (nz - 1) + sides

    def place(g, lag):
        g = g - lag
        ok = (g >= 0) & (g < count * period)
        g = jnp.clip(g, 0, count * period - 1)
        return ok, g // period, lax.rem(g, period)

    def one(it, carry):
        sent, gone = carry
        g = it - LEAD
        ok, t, p = place(g, -LEAD)

        @pl.when(ok & (t == 0) & (p == 0))
        def _():
            first_copy(0).wait()

        @pl.when(ok & (t == 0) & (p == LEAD + 2))
        def _():
            for c in rest:
                c.start()
            each(1, nz, lambda i: first_copy(i).wait())

        @pl.when(ok & (t == 1) & (p == 0))
        def _():
            rest[0].wait()

        ok, t, p = place(g, lag_a)
        i, j = jnp.minimum(p // tall, nz - 2), lax.rem(p, tall)

        live = ok & (p < tall * (nz - 1)) & (j < 2 * n_a(order(i)))

        @pl.when(live)
        def _():
            a_job(t, i, j, gone)
        gone = gone + jnp.where(live, 1, 0)

        ok, t, p = place(g, 0)
        tail = p >= own
        i = jnp.where(tail, nz - 1, p // wide)
        c = jnp.where(tail, p - own, lax.rem(p, wide))
        live = ok & (tail | (p < own - sides)) & (c < n_b(order(i)))

        @pl.when(live)
        def _():
            y_job(t, i, c, lax.rem(sent, RING), sent >= RING)
        sent = sent + jnp.where(live, 1, 0)
        c = p - (own - sides)

        @pl.when(ok & (c >= 0) & (c < n_a(z)) & (p < own))
        def _():
            s_job(t, c)

        ok, t, p = place(g, lag_b)
        i, c = p // wide, lax.rem(p, wide)

        live = ok & (p < own - sides) & (c < n_b(order(i)))

        @pl.when(live)
        def _():
            b_job(t, i, c, gone)
        gone = gone + jnp.where(live, 1, 0)

        ok, t, p = place(g, LAG_UPDATE)
        c = p - (own - sides)

        @pl.when(ok & (c >= 0) & (c < n_a(z)) & (p < own))
        def _():
            update_a(t, c)
        c = p - own

        @pl.when(ok & (c >= 0) & (c < n_b(z)))
        def _():
            update_b(t, c)

        @pl.when(ok & (p == period - 1) & (t < count - 1))
        def _():
            share(t)

        ok, t, p = place(g, LAG_UPDATE + LAG_FINISH)

        @pl.when(ok & (p == period - 1))
        def _():
            finish(t)
        return sent, gone

    lax.fori_loop(0, LEAD + count * period + LAG_UPDATE, one, (0, 0))
    share(count - 1)
    rows_of(count - 1).wait_recv()

    each(0, RING, lambda r: y_copy(0, 0, 0, r).wait_send())

    each(0, Z_RING, lambda r: z_sent(z_send.at[r]))
    each(0, n_a(z), lambda c: s_copy(0, c).wait_send())
    for t in range(max(0, count - 2), count):
        rows_of(t).wait_send()


def last(n, par, qm, qv, m_new, v_new, old, row, row_in, out_p, out_m, out_v, out_scale, out_top, out_exp,
         qm_last, qv_last, stats, scale, top, exp, sem):
    count, rows, width = par.shape
    groups = out_top.shape[0]
    lanes = width // groups
    t = count - 1
    h = t % 2
    copies = [pltpu.make_async_copy(par, out_p, sem.at[0])]
    for i, (src, dst) in enumerate(((qm, out_m), (qv, out_v))):
        copies.append(pltpu.make_async_copy(src.at[pl.ds(0, t)], dst.at[pl.ds(0, t)], sem.at[1 + i]))
    for c in copies:
        c.start()
    stats[pl.ds(0, t)] = old[pl.ds(0, t)]
    inverse, exps, invs = merged(n, groups, row, row_in, stats, t, h)
    lane = lax.broadcasted_iota(jnp.int32, (1, lanes), 1)

    def packed(k):
        line = stats[0, k:k + 1, :]
        for u in range(1, count):
            line = jnp.where(lane == u, stats[u, k:k + 1, :], line)
        return line[:, :count]
    scale[...] = packed(0)
    for g in range(groups):
        top[g:g + 1, :] = packed(1 + g)
        exp[g:g + 1, :] = packed(1 + groups + g)
    for i, (src, dst) in enumerate(((scale, out_scale), (top, out_top), (exp, out_exp))):
        c = pltpu.make_async_copy(src, dst, sem.at[3 + i])
        c.start()
        copies.append(c)

    def body(i, _):
        at = pl.ds(pl.multiple_of(i * LONG, LONG), LONG)
        for g in range(groups):
            cols = slice(g * lanes, (g + 1) * lanes)
            value = jnp.exp(exps[g] * jnp.log(v_new[h, at, cols] * invs[g]))
            qv_last[at, cols] = value.astype(jnp.bfloat16)
            qm_last[at, cols] = (m_new[h, at, cols] * inverse).astype(jnp.bfloat16)
        return 0
    lax.fori_loop(0, rows // LONG, body, 0)
    for i, (src, dst) in enumerate(((qm_last, out_m), (qv_last, out_v))):
        c = pltpu.make_async_copy(src, dst.at[t], sem.at[6 + i])
        c.start()
        copies.append(c)
    for c in copies:
        c.wait()


def on_device(n, peers, grads, param, q_m, m_scale, q_v, v_max, v_exp):
    count, rows, width = q_m.shape
    groups = v_max.shape[1]
    lanes = width // groups
    nz = n // 2
    chunk = rows // (8 * SPLIT)
    wide, tall, deep = 7 * SPLIT, 4 * SPLIT, 10 * SPLIT
    kinds = -(-(1 + 2 * groups) // 8) * 8
    f32, bf16 = jnp.float32, jnp.bfloat16
    dma = pltpu.SemaphoreType.DMA
    hbm = pl.BlockSpec(memory_space=pl.ANY)
    smem = pl.BlockSpec(memory_space=pltpu.SMEM)
    vmem = pl.BlockSpec(memory_space=pltpu.VMEM)
    buffers = [
        pltpu.VMEM((count, n, rows, width), bf16),
        pltpu.VMEM((RING, chunk, width), f32),
        pltpu.VMEM((nz - 1, tall, chunk, width), f32),
        pltpu.VMEM((SLOTS, nz, wide, chunk, width), f32),
        pltpu.VMEM((SLOTS, 2 * (nz - 2), deep, chunk, width), f32),
        pltpu.VMEM((2 * SPLIT, chunk, width), f32),
        pltpu.VMEM((SLOTS, 2 * SPLIT, chunk, width), f32),
        pltpu.VMEM((count, kinds, lanes), f32),
    ]
    grant = SPARE + sum(math.prod(b.shape) * b.dtype.itemsize for b in buffers)
    state = pl.pallas_call(
        functools.partial(kernel, n, peers),
        out_shape=(
            pltpu.VMEM(param.shape, f32),
            pltpu.VMEM(q_m.shape, bf16),
            pltpu.VMEM(q_v.shape, bf16),
            pltpu.VMEM((2, rows, width), f32),
            pltpu.VMEM((2, rows, width), f32),
            pltpu.VMEM((count, kinds, lanes), f32),
            pltpu.VMEM((2, 1, lanes), f32),
            pltpu.VMEM((2, n * peers, 1, lanes), f32),
        ),
        in_specs=[hbm] * 4 + [smem] * 3,
        out_specs=[vmem] * 8,
        scratch_shapes=buffers + [
            dma((nz,)), dma((4,)),
            dma((RING,)), dma((nz, wide)),
            dma((Z_RING,)), dma((2, 2 * (nz - 2), deep)),
            dma((2 * SPLIT,)), dma((2 * SPLIT,)),
            dma((2,)), dma((2,)),
        ],
        compiler_params=pltpu.CompilerParams(
            collective_id=0, has_side_effects=True, vmem_limit_bytes=grant
        ),
    )(grads[0].reshape(count, n, rows, width), param, q_m, q_v, m_scale, v_max.T, v_exp.T)
    new_param, new_q_m, new_q_v, scales, tops, exps = pl.pallas_call(
        functools.partial(last, n),
        out_shape=(
            jax.ShapeDtypeStruct(param.shape, f32),
            jax.ShapeDtypeStruct(q_m.shape, bf16),
            jax.ShapeDtypeStruct(q_v.shape, bf16),
            jax.ShapeDtypeStruct((1, count), f32),
            jax.ShapeDtypeStruct((groups, count), f32),
            jax.ShapeDtypeStruct((groups, count), f32),
        ),
        in_specs=[vmem] * 8,
        out_specs=[hbm] * 6,
        scratch_shapes=[
            pltpu.VMEM((rows, width), bf16),
            pltpu.VMEM((rows, width), bf16),
            pltpu.VMEM((count, kinds, lanes), f32),
            pltpu.VMEM((1, count), f32),
            pltpu.VMEM((groups, count), f32),
            pltpu.VMEM((groups, count), f32),
            dma((8,)),
        ],
        compiler_params=pltpu.CompilerParams(vmem_limit_bytes=4 << 20),
    )(*state)
    return new_param, new_q_m, scales.reshape(count), new_q_v, tops.T, exps.T


def solution(mesh):
    in_specs = (
        P("dp", None, None, "tensor"),
        P(None, "dp", "tensor"),
        P(None, "dp", "tensor"),
        P(),
        P(None, "dp", "tensor"),
        P(None, "tensor"),
        P(None, "tensor"),
    )
    out_specs = (
        P(None, "dp", "tensor"),
        P(None, "dp", "tensor"),
        P(),
        P(None, "dp", "tensor"),
        P(None, "tensor"),
        P(None, "tensor"),
    )
    return jax.shard_map(
        functools.partial(on_device, mesh.shape["dp"], mesh.shape["tensor"]),
        mesh=mesh, in_specs=in_specs, out_specs=out_specs, check_vma=False
    )
```

```python
import functools
import math

import jax
import jax.numpy as jnp
from jax import lax
from jax.experimental import pallas as pl
from jax.experimental.pallas import tpu as pltpu
from jax.sharding import PartitionSpec as P

MESH = pl.DeviceIdType.MESH
STEP = 32
LONG = 128
SPLIT = 1
SLOTS = 3
RING = 4
Z_RING = 16
LEAD = 0
CHAIN_AT = 3
LAG_A = 4
LAG_B = 5
LAG_B_INNER = 9
LAG_UPDATE = 5
LAG_FINISH = 10
SPARE = 1 << 20


def merged(n, groups, row, row_in, out, t, h):
    lane = lax.broadcasted_iota(jnp.int32, row.shape[1:], 1)

    def pick(line, k):
        return jnp.broadcast_to(jnp.max(jnp.where(lane == k, line, -jnp.inf), axis=1, keepdims=True), line.shape)
    best = jnp.maximum(row[h], jnp.max(row_in[h, pl.ds(1, n - 1)], axis=0))
    every = jnp.maximum(best, jnp.max(row_in[h, pl.ds(n, row_in.shape[1] - n)], axis=0))
    whole = pick(every, 0) + 1e-06
    out[t, 0:1, :] = whole
    exps, invs = [], []
    for g in range(groups):
        top = pick(best, 1 + g)
        low = -pick(best, 1 + groups + g)
        exps.append(12.343 / jnp.maximum(jnp.log(top / low), 1.0))
        invs.append(1.0 / top)
        out[t, 1 + g:2 + g, :] = top
        out[t, 1 + groups + g:2 + groups + g, :] = exps[g]
    return 1.0 / whole, exps, invs


def kernel(n, peers, *refs):
    (grads, param, q_m, q_v, m_scale, v_max, v_exp,
     par, qm, qv, m_new, v_new, out_s, row, row_in,
     raw, y_cast, a_cast, y_in, z_in, s_out, s_in,
     stat,
     first_sem, rest_sem, token, y_send, y_recv, z_send, z_recv, s_send, s_recv,
     st_send, st_recv) = refs
    count, _, rows, width = grads.shape
    groups = v_max.shape[0]
    lanes = width // groups
    nz = n // 2
    chunk = rows // (8 * SPLIT)
    step = min(STEP, chunk)
    wide = 7 * SPLIT
    tall = 4 * SPLIT
    sides = 2 * SPLIT
    period = wide * nz + sides
    me = lax.axis_index("dp")
    mt = lax.axis_index("tensor")
    y = lax.rem(me, 2)
    z = me // 2
    half = z // (nz // 2)
    zm = z + half * (nz - 1 - 2 * z)
    is_outer = zm == 0
    is_inner = zm == 1
    inner = 1 + half * (nz - 3)

    def is_end(d):
        return 1 - (lax.rem(d, nz - 1) + nz - 2) // (nz - 1)

    def n_b(d):
        return SPLIT * (7 - is_end(d))

    def n_a(d):
        return SPLIT * (1 + is_end(d))

    def order(i):
        low = jnp.minimum(zm, 1)
        d = nz - 1 + low - i
        d = d - low * jnp.where(d <= zm, 1, 0)
        d = jnp.where((i == 0) & (zm > 0), 0, d)
        d = jnp.where(i == nz - 1, zm, d)
        return d + half * (nz - 1 - 2 * d)

    def through(d):
        return nz - 2 + d - 2 * (1 - half)

    barrier = pltpu.get_barrier_semaphore()

    def first_copy(i, lo=0, sem=None):
        at = (0, pl.ds(order(i) * 2, 2), pl.ds(lo, chunk if sem is not None else rows - lo))
        return pltpu.make_async_copy(grads.at[at], raw.at[at], first_sem.at[i if sem is None else sem])

    later = pl.ds(1, count - 1)
    rest = [pltpu.make_async_copy(src, dst, rest_sem.at[i]) for i, (src, dst) in enumerate((
        (grads.at[later], raw.at[later]), (q_m, qm), (q_v, qv), (param, par)))]
    first_copy(0, 0, nz).start()
    first_copy(0, chunk).start()

    def each(lo, hi, act):
        def one(o, _):
            act(o)
            return 0
        lax.fori_loop(lo, hi, one, 0)

    def greet(axis, to):
        pl.semaphore_signal(barrier, inc=1, device_id={axis: to}, device_id_type=MESH)

    def beside(step):
        return {"dp": (z + step) * 2 + y}
    first, final = z == 0, z == nz - 1
    greet("dp", z * 2 + 1 - y)

    @pl.when(jnp.logical_not(first))
    def _():
        greet("dp", (z - 1) * 2 + y)

    @pl.when(jnp.logical_not(final))
    def _():
        greet("dp", (z + 1) * 2 + y)
    each(1, peers, lambda o: greet("tensor", lax.rem(mt + o, peers)))
    each(1, nz, lambda i: first_copy(i).start())
    pl.semaphore_wait(barrier, peers + 2 - jnp.where(first | final, 1, 0))

    def tell(side, step):
        pl.semaphore_signal(token.at[side], inc=1, device_id=beside(step), device_id_type=MESH)

    def chain():
        @pl.when(first)
        def _():
            tell(0, 1)

        @pl.when(final)
        def _():
            tell(1, -1)

        @pl.when(jnp.logical_not(first))
        def _():
            pl.semaphore_wait(token.at[0], 1)

            @pl.when(jnp.logical_not(final))
            def _():
                tell(0, 1)

        @pl.when(jnp.logical_not(final))
        def _():
            pl.semaphore_wait(token.at[1], 1)

            @pl.when(jnp.logical_not(first))
            def _():
                tell(1, -1)
    if nz > 4:
        chain()

    def remote(src, dst, s_sem, r_sem, to):
        return pltpu.make_async_remote_copy(src_ref=src, dst_ref=dst, send_sem=s_sem, recv_sem=r_sem,
                                            device_id={"dp": to}, device_id_type=MESH)

    def loop(body):
        def one(i, _):
            body(pl.ds(pl.multiple_of(i * step, step), step))
            return 0
        lax.fori_loop(0, chunk // step, one, 0)

    def mine(t, d, side, c, at):
        first = pl.multiple_of(c * chunk + at.start, step)
        return raw[t, d * 2 + side, pl.ds(first, step), :].astype(jnp.float32)

    def y_copy(t, d, c, ring):
        s = lax.rem(t, SLOTS)
        return remote(y_cast.at[ring], y_in.at[s, d, c], y_send.at[ring], y_recv.at[d, c], z * 2 + 1 - y)

    def s_copy(t, c):
        s = lax.rem(t, SLOTS)
        return remote(s_out.at[c], s_in.at[s, c], s_send.at[c], s_recv.at[c], z * 2 + 1 - y)

    def z_wait(t, where, c):
        s = lax.rem(t, SLOTS)
        remote(z_in.at[s, where, c], z_in.at[s, where, c], z_send.at[0], z_recv.at[lax.rem(t, 2), where, c], me).wait_recv()

    def landed(t, c):
        for k in range(nz - 2):
            if nz > 4:
                @pl.when((zm <= 1) | (z != k + 1))
                def _():
                    z_wait(t, k, c)
            else:
                z_wait(t, k, c)

    def gathered(t, c, at):
        s = lax.rem(t, SLOTS)
        total = None
        for k in range(nz - 2):
            part = z_in[s, k, c, at, :]
            if nz > 4:
                part = jnp.where((zm <= 1) | (z != k + 1), part, 0.0)
            total = part if total is None else total + part
        return total

    def z_go(t, src, d, c, sem):
        s = lax.rem(t, SLOTS)
        to = jnp.where(is_outer, inner, d)
        where = jnp.where(is_outer, jnp.where(d == inner, d - 1, through(d)), z - 1)
        remote(src, z_in.at[s, where, c], sem, z_recv.at[lax.rem(t, 2), where, c], to * 2 + y).start()

    def z_sent(sem):
        remote(a_cast.at[0, 0], a_cast.at[0, 0], sem, z_recv.at[0, 0, 0], me).wait_send()

    def y_job(t, i, c, ring, full):
        d = order(i)

        @pl.when(full)
        def _():
            y_copy(t, d, c, ring).wait_send()

        def body(at):
            y_cast[ring, at, :] = mine(t, d, 1 - y, c, at)
        loop(body)
        y_copy(t, d, c, ring).start()

    def s_job(t, c):
        @pl.when(t > 0)
        def _():
            s_copy(t, c).wait_send()
        j = n_b(z) + (1 - y) * n_a(z) + c
        landed(t, j)

        def body(at):
            s_out[c, at, :] = gathered(t, j, at) + mine(t, z, 1 - y, n_b(z) + c, at)
        loop(body)
        s_copy(t, c).start()

    def a_job(t, i, j, gone):
        s = lax.rem(t, SLOTS)
        d = order(i)
        side = j // n_a(d)
        c = n_b(d) + lax.rem(j, n_a(d))
        k = n_b(d) + j
        sem = z_send.at[lax.rem(gone, Z_RING)]

        @pl.when(gone >= Z_RING)
        def _():
            z_sent(sem)
        relay = is_inner & (i > 0)

        @pl.when(relay)
        def _():
            w = through(d)
            z_wait(t, w, k)

            def body(at):
                z_in[s, w, k, at, :] = z_in[s, w, k, at, :] + mine(t, d, side, c, at)
            loop(body)
            z_go(t, z_in.at[s, w, k], d, k, sem)

        @pl.when(jnp.logical_not(relay))
        def _():
            def body(at):
                a_cast[i, j, at, :] = mine(t, d, side, c, at)
            loop(body)
            z_go(t, a_cast.at[i, j], d, k, sem)

    def b_job(t, i, c, gone):
        s = lax.rem(t, SLOTS)
        d = order(i)
        sem = z_send.at[lax.rem(gone, Z_RING)]

        @pl.when(gone >= Z_RING)
        def _():
            z_sent(sem)
        y_copy(t, d, c, 0).wait_recv()
        relay = is_inner & (i > 0)

        @pl.when(relay)
        def _():
            w = through(d)
            z_wait(t, w, c)

            def body(at):
                z_in[s, w, c, at, :] = z_in[s, w, c, at, :] + (y_in[s, d, c, at, :] + mine(t, d, y, c, at))
            loop(body)
            z_go(t, z_in.at[s, w, c], d, c, sem)

        @pl.when(jnp.logical_not(relay))
        def _():
            def body(at):
                y_in[s, d, c, at, :] = y_in[s, d, c, at, :] + mine(t, d, y, c, at)
            loop(body)
            z_go(t, y_in.at[s, d, c], d, c, sem)

    def update(t, c, total):
        scale = m_scale[t]
        h = lax.rem(t, 2)

        def fold(x):
            return jnp.max(x.reshape(step // 8, 8, lanes), axis=0)

        def one(it, carry):
            at = pl.ds(pl.multiple_of(it * step, step), step)
            whole = total(at) * (1.0 / n)
            rows_i = pl.ds(pl.multiple_of(c * chunk + it * step, step), step)
            top_m, tops, lows = carry
            new_tops, new_lows = [], []
            for g in range(groups):
                cols = slice(g * lanes, (g + 1) * lanes)
                grad = whole[:, cols]
                m_old = scale * qm[t, rows_i, cols].astype(jnp.float32)
                stored = qv[t, rows_i, cols].astype(jnp.float32)
                inv = 1.0 / jnp.full((1, lanes), v_exp[g, t], jnp.float32)
                v_old = v_max[g, t] * jnp.exp(jnp.log(stored) * inv)
                m = 0.9 * m_old + 0.1 * grad
                v = 0.95 * v_old + 0.05 * grad * grad
                w = par[t, rows_i, cols]
                par[t, rows_i, cols] = w - 0.02 * (m / (jnp.sqrt(v) + 1e-08) + 0.1 * w)
                m_new[h, rows_i, cols] = m
                v_new[h, rows_i, cols] = v
                top_m = jnp.maximum(top_m, fold(jnp.abs(m)))
                new_tops.append(jnp.maximum(tops[g], fold(v)))
                new_lows.append(jnp.maximum(lows[g], fold(-v)))
            return top_m, tuple(new_tops), tuple(new_lows)
        least = jnp.full((8, lanes), -jnp.inf, jnp.float32)
        top_m, tops, lows = lax.fori_loop(0, chunk // step, one, (least, (least,) * groups, (least,) * groups))
        for row, value in enumerate((top_m,) + tops + lows):
            stat[t, row:row + 1, :] = jnp.maximum(stat[t, row:row + 1, :], jnp.max(value, axis=0, keepdims=True))

    def update_a(t, c):
        s = lax.rem(t, SLOTS)

        @pl.when((c == 0) & (t == 0))
        def _():
            for copy in rest[1:]:
                copy.wait()

        @pl.when(c == 0)
        def _():
            stat[t] = jnp.full(stat.shape[1:], -jnp.inf, jnp.float32)
        j = n_b(z) + y * n_a(z) + c
        landed(t, j)
        s_copy(t, c).wait_recv()
        update(t, n_b(z) + c,
               lambda at: gathered(t, j, at) + mine(t, z, y, n_b(z) + c, at) + s_in[s, c, at, :])

    def update_b(t, c):
        s = lax.rem(t, SLOTS)
        y_copy(t, z, c, 0).wait_recv()
        landed(t, c)
        update(t, c, lambda at: gathered(t, c, at) + (y_in[s, z, c, at, :] + mine(t, z, y, c, at)))

    def row_copy(t, o):
        h = lax.rem(t, 2)
        return pltpu.make_async_remote_copy(
            src_ref=row.at[h], dst_ref=row_in.at[h, o], send_sem=st_send.at[h], recv_sem=st_recv.at[h],
            device_id={"tensor": lax.rem(mt + o // n, peers), "dp": lax.rem(me + lax.rem(o, n), n)},
            device_id_type=MESH)

    def rows_of(t):
        h = lax.rem(t, 2)
        part = row_in.at[h, pl.ds(1, n * peers - 1)]
        return remote(part, part, st_send.at[h], st_recv.at[h], me)

    kinds = stat.shape[1]

    def share(t):
        h = lax.rem(t, 2)
        if not isinstance(t, int) or t >= 2:
            @pl.when(t >= 2)
            def _():
                rows_of(t).wait_send()
        best = jnp.broadcast_to(jnp.max(stat[t], axis=1, keepdims=True), (kinds, lanes))
        at = [lax.broadcasted_iota(jnp.int32, (kinds, lanes), i) for i in range(2)]
        row[h] = jnp.max(jnp.where(at[0] == at[1], best, -jnp.inf), axis=0, keepdims=True)
        each(1, n * peers, lambda o: row_copy(t, n * peers - o).start())

    def all_rows(body):
        def one(i, _):
            body(pl.ds(pl.multiple_of(i * LONG, LONG), LONG))
            return 0
        lax.fori_loop(0, rows // LONG, one, 0)

    def finish(t):
        h = lax.rem(t, 2)
        rows_of(t).wait_recv()
        inverse, exps, invs = merged(n, groups, row, row_in, out_s, t, h)

        def body(at):
            for g in range(groups):
                cols = slice(g * lanes, (g + 1) * lanes)
                value = jnp.exp(exps[g] * jnp.log(v_new[h, at, cols] * invs[g]))
                qv[t, at, cols] = value.astype(jnp.bfloat16)
                qm[t, at, cols] = (m_new[h, at, cols] * inverse).astype(jnp.bfloat16)
        all_rows(body)

    lag_a = jnp.where(is_inner, LAG_A, -LEAD)
    lag_b = jnp.where(is_inner, LAG_B_INNER, LAG_B)
    own = wide * (nz - 1) + sides

    def place(g, lag):
        g = g - lag
        ok = (g >= 0) & (g < count * period)
        g = jnp.clip(g, 0, count * period - 1)
        return ok, g // period, lax.rem(g, period)

    def one(it, carry):
        sent, gone = carry
        g = it - LEAD
        ok, t, p = place(g, -LEAD)

        @pl.when(ok & (t == 0) & (p == 0))
        def _():
            first_copy(0, 0, nz).wait()

        @pl.when(ok & (t == 0) & (p == LEAD + 2))
        def _():
            for c in rest:
                c.start()
            each(1, nz, lambda i: first_copy(i).wait())

        if nz == 4:
            @pl.when(g == CHAIN_AT)
            def _():
                chain()

        @pl.when(ok & (t == 1) & (p == 0))
        def _():
            rest[0].wait()

        ok, t, p = place(g, 0)
        tail = p >= own
        i = jnp.where(tail, nz - 1, p // wide)
        c = jnp.where(tail, p - own, lax.rem(p, wide))
        live = ok & (tail | (p < own - sides)) & (c < n_b(order(i)))

        @pl.when(live)
        def _():
            y_job(t, i, c, lax.rem(sent, RING), sent >= RING)
        sent = sent + jnp.where(live, 1, 0)
        c = p - (own - sides)

        @pl.when(ok & (c >= 0) & (c < n_a(z)) & (p < own))
        def _():
            s_job(t, c)

        @pl.when(g == 0)
        def _():
            first_copy(0, chunk).wait()

        ok, t, p = place(g, lag_a)
        i, j = jnp.minimum(p // tall, nz - 2), lax.rem(p, tall)

        live = ok & (p < tall * (nz - 1)) & (j < 2 * n_a(order(i)))

        @pl.when(live)
        def _():
            a_job(t, i, j, gone)
        gone = gone + jnp.where(live, 1, 0)

        ok, t, p = place(g, lag_b)
        i, c = p // wide, lax.rem(p, wide)

        live = ok & (p < own - sides) & (c < n_b(order(i)))

        @pl.when(live)
        def _():
            b_job(t, i, c, gone)
        gone = gone + jnp.where(live, 1, 0)

        ok, t, p = place(g, LAG_UPDATE)
        c = p - (own - sides)

        @pl.when(ok & (c >= 0) & (c < n_a(z)) & (p < own))
        def _():
            update_a(t, c)
        c = p - own

        @pl.when(ok & (c >= 0) & (c < n_b(z)))
        def _():
            update_b(t, c)

        @pl.when(ok & (p == period - 1) & (t < count - 1))
        def _():
            share(t)

        ok, t, p = place(g, LAG_UPDATE + LAG_FINISH)

        @pl.when(ok & (p == period - 1))
        def _():
            finish(t)
        return sent, gone

    lax.fori_loop(0, LEAD + count * period + LAG_UPDATE, one, (0, 0))
    share(count - 1)

    each(0, RING, lambda r: y_copy(0, 0, 0, r).wait_send())
    each(0, Z_RING, lambda r: z_sent(z_send.at[r]))
    each(0, n_a(z), lambda c: s_copy(0, c).wait_send())
    for t in range(max(0, count - 2), count):
        rows_of(t).wait_send()
    rows_of(count - 1).wait_recv()


def last(n, par, qm, qv, m_new, v_new, old, row, row_in, out_p, out_m, out_v, out_scale, out_top, out_exp,
         qm_last, qv_last, stats, scale, top, exp, sem):
    count, rows, width = par.shape
    groups = out_top.shape[0]
    lanes = width // groups
    t = count - 1
    h = t % 2
    copies = [pltpu.make_async_copy(par, out_p, sem.at[0])]
    for i, (src, dst) in enumerate(((qm, out_m), (qv, out_v))):
        copies.append(pltpu.make_async_copy(src.at[pl.ds(0, t)], dst.at[pl.ds(0, t)], sem.at[1 + i]))
    for c in copies:
        c.start()
    stats[pl.ds(0, t)] = old[pl.ds(0, t)]
    inverse, exps, invs = merged(n, groups, row, row_in, stats, t, h)
    lane = lax.broadcasted_iota(jnp.int32, (1, lanes), 1)

    def packed(k):
        line = stats[0, k:k + 1, :]
        for u in range(1, count):
            line = jnp.where(lane == u, stats[u, k:k + 1, :], line)
        return line[:, :count]
    scale[...] = packed(0)
    for g in range(groups):
        top[g:g + 1, :] = packed(1 + g)
        exp[g:g + 1, :] = packed(1 + groups + g)
    for i, (src, dst) in enumerate(((scale, out_scale), (top, out_top), (exp, out_exp))):
        c = pltpu.make_async_copy(src, dst, sem.at[3 + i])
        c.start()
        copies.append(c)

    def body(i, _):
        at = pl.ds(pl.multiple_of(i * LONG, LONG), LONG)
        for g in range(groups):
            cols = slice(g * lanes, (g + 1) * lanes)
            value = jnp.exp(exps[g] * jnp.log(v_new[h, at, cols] * invs[g]))
            qv_last[at, cols] = value.astype(jnp.bfloat16)
            qm_last[at, cols] = (m_new[h, at, cols] * inverse).astype(jnp.bfloat16)
        return 0
    lax.fori_loop(0, rows // LONG, body, 0)
    for i, (src, dst) in enumerate(((qm_last, out_m), (qv_last, out_v))):
        c = pltpu.make_async_copy(src, dst.at[t], sem.at[6 + i])
        c.start()
        copies.append(c)
    for c in copies:
        c.wait()


def on_device(n, peers, grads, param, q_m, m_scale, q_v, v_max, v_exp):
    count, rows, width = q_m.shape
    groups = v_max.shape[1]
    lanes = width // groups
    nz = n // 2
    chunk = rows // (8 * SPLIT)
    wide, tall, deep = 7 * SPLIT, 4 * SPLIT, 10 * SPLIT
    kinds = -(-(1 + 2 * groups) // 8) * 8
    f32, bf16 = jnp.float32, jnp.bfloat16
    dma = pltpu.SemaphoreType.DMA
    hbm = pl.BlockSpec(memory_space=pl.ANY)
    smem = pl.BlockSpec(memory_space=pltpu.SMEM)
    vmem = pl.BlockSpec(memory_space=pltpu.VMEM)
    buffers = [
        pltpu.VMEM((count, n, rows, width), bf16),
        pltpu.VMEM((RING, chunk, width), f32),
        pltpu.VMEM((nz - 1, tall, chunk, width), f32),
        pltpu.VMEM((SLOTS, nz, wide, chunk, width), f32),
        pltpu.VMEM((SLOTS, 2 * (nz - 2), deep, chunk, width), f32),
        pltpu.VMEM((2 * SPLIT, chunk, width), f32),
        pltpu.VMEM((SLOTS, 2 * SPLIT, chunk, width), f32),
        pltpu.VMEM((count, kinds, lanes), f32),
    ]
    grant = SPARE + sum(math.prod(b.shape) * b.dtype.itemsize for b in buffers)
    state = pl.pallas_call(
        functools.partial(kernel, n, peers),
        out_shape=(
            pltpu.VMEM(param.shape, f32),
            pltpu.VMEM(q_m.shape, bf16),
            pltpu.VMEM(q_v.shape, bf16),
            pltpu.VMEM((2, rows, width), f32),
            pltpu.VMEM((2, rows, width), f32),
            pltpu.VMEM((count, kinds, lanes), f32),
            pltpu.VMEM((2, 1, lanes), f32),
            pltpu.VMEM((2, n * peers, 1, lanes), f32),
        ),
        in_specs=[hbm] * 4 + [smem] * 3,
        out_specs=[vmem] * 8,
        scratch_shapes=buffers + [
            dma((nz + 1,)), dma((4,)), pltpu.SemaphoreType.REGULAR((2,)),
            dma((RING,)), dma((nz, wide)),
            dma((Z_RING,)), dma((2, 2 * (nz - 2), deep)),
            dma((2 * SPLIT,)), dma((2 * SPLIT,)),
            dma((2,)), dma((2,)),
        ],
        compiler_params=pltpu.CompilerParams(
            collective_id=0, has_side_effects=True, vmem_limit_bytes=grant
        ),
    )(grads[0].reshape(count, n, rows, width), param, q_m, q_v, m_scale, v_max.T, v_exp.T)
    new_param, new_q_m, new_q_v, scales, tops, exps = pl.pallas_call(
        functools.partial(last, n),
        out_shape=(
            jax.ShapeDtypeStruct(param.shape, f32),
            jax.ShapeDtypeStruct(q_m.shape, bf16),
            jax.ShapeDtypeStruct(q_v.shape, bf16),
            jax.ShapeDtypeStruct((1, count), f32),
            jax.ShapeDtypeStruct((groups, count), f32),
            jax.ShapeDtypeStruct((groups, count), f32),
        ),
        in_specs=[vmem] * 8,
        out_specs=[hbm] * 6,
        scratch_shapes=[
            pltpu.VMEM((rows, width), bf16),
            pltpu.VMEM((rows, width), bf16),
            pltpu.VMEM((count, kinds, lanes), f32),
            pltpu.VMEM((1, count), f32),
            pltpu.VMEM((groups, count), f32),
            pltpu.VMEM((groups, count), f32),
            dma((8,)),
        ],
        compiler_params=pltpu.CompilerParams(vmem_limit_bytes=4 << 20),
    )(*state)
    return new_param, new_q_m, scales.reshape(count), new_q_v, tops.T, exps.T


def solution(mesh):
    in_specs = (
        P("dp", None, None, "tensor"),
        P(None, "dp", "tensor"),
        P(None, "dp", "tensor"),
        P(),
        P(None, "dp", "tensor"),
        P(None, "tensor"),
        P(None, "tensor"),
    )
    out_specs = (
        P(None, "dp", "tensor"),
        P(None, "dp", "tensor"),
        P(),
        P(None, "dp", "tensor"),
        P(None, "tensor"),
        P(None, "tensor"),
    )
    return jax.shard_map(
        functools.partial(on_device, mesh.shape["dp"], mesh.shape["tensor"]),
        mesh=mesh, in_specs=in_specs, out_specs=out_specs, check_vma=False
    )
```

```python
import functools
import math

import jax
import jax.numpy as jnp
from jax import lax
from jax.experimental import pallas as pl
from jax.experimental.pallas import tpu as pltpu
from jax.sharding import PartitionSpec as P

MESH = pl.DeviceIdType.MESH
STEP = 32
LONG = 128
SPLIT = 1
SLOTS = 3
RING = 4
Z_RING = 12
LEAD = 0
CHAIN_AT = 3
LAG_A = 4
LAG_B = 5
LAG_B_INNER = 9
LAG_UPDATE = 5
LAG_FINISH = 10
SPARE = 1 << 20


def merged(n, groups, row, row_in, out, t, h):
    lane = lax.broadcasted_iota(jnp.int32, row.shape[1:], 1)

    def pick(line, k):
        return jnp.broadcast_to(jnp.max(jnp.where(lane == k, line, -jnp.inf), axis=1, keepdims=True), line.shape)
    best = jnp.maximum(row[h], jnp.max(row_in[h, pl.ds(1, n - 1)], axis=0))
    every = jnp.maximum(best, jnp.max(row_in[h, pl.ds(n, row_in.shape[1] - n)], axis=0))
    whole = pick(every, 0) + 1e-06
    out[t, 0:1, :] = whole
    exps, invs = [], []
    for g in range(groups):
        top = pick(best, 1 + g)
        low = -pick(best, 1 + groups + g)
        exps.append(12.343 / jnp.maximum(jnp.log(top / low), 1.0))
        invs.append(1.0 / top)
        out[t, 1 + g:2 + g, :] = top
        out[t, 1 + groups + g:2 + groups + g, :] = exps[g]
    return 1.0 / whole, exps, invs


def kernel(n, peers, *refs):
    (grads, param, q_m, q_v, m_scale, v_max, v_exp,
     par, qm, qv, m_new, v_new, out_s, row, row_in,
     raw, y_cast, a_cast, y_in, z_in, s_out, s_in,
     stat,
     first_sem, rest_sem, token, y_send, y_recv, z_send, z_recv, s_send, s_recv,
     st_send, st_recv) = refs
    count, _, rows, width = grads.shape
    groups = v_max.shape[0]
    lanes = width // groups
    nz = n // 2
    chunk = rows // (8 * SPLIT)
    step = min(STEP, chunk)
    wide = 7 * SPLIT
    tall = 4 * SPLIT
    sides = 2 * SPLIT
    period = wide * nz + sides
    me = lax.axis_index("dp")
    mt = lax.axis_index("tensor")
    y = lax.rem(me, 2)
    z = me // 2
    half = z // (nz // 2)
    zm = z + half * (nz - 1 - 2 * z)
    is_outer = zm == 0
    is_inner = zm == 1
    inner = 1 + half * (nz - 3)

    def is_end(d):
        return 1 - (lax.rem(d, nz - 1) + nz - 2) // (nz - 1)

    def n_b(d):
        return SPLIT * (7 - is_end(d))

    def n_a(d):
        return SPLIT * (1 + is_end(d))

    def order(i):
        low = jnp.minimum(zm, 1)
        d = nz - 1 + low - i
        d = d - low * jnp.where(d <= zm, 1, 0)
        d = jnp.where((i == 0) & (zm > 0), 0, d)
        d = jnp.where(i == nz - 1, zm, d)
        return d + half * (nz - 1 - 2 * d)

    def through(d):
        return nz - 2 + d - 2 * (1 - half)

    barrier = pltpu.get_barrier_semaphore()

    def first_copy(i, lo=0, sem=None):
        at = (0, pl.ds(order(i) * 2, 2), pl.ds(lo, chunk if sem is not None else rows - lo))
        return pltpu.make_async_copy(grads.at[at], raw.at[at], first_sem.at[i if sem is None else sem])

    later = pl.ds(1, count - 1)
    rest = [pltpu.make_async_copy(src, dst, rest_sem.at[i]) for i, (src, dst) in enumerate((
        (grads.at[later], raw.at[later]), (q_m, qm), (q_v, qv), (param, par)))]
    first_copy(0, 0, nz).start()
    first_copy(0, chunk).start()

    def each(lo, hi, act):
        def one(o, _):
            act(o)
            return 0
        lax.fori_loop(lo, hi, one, 0)

    def greet(axis, to):
        pl.semaphore_signal(barrier, inc=1, device_id={axis: to}, device_id_type=MESH)

    def beside(step):
        return {"dp": (z + step) * 2 + y}
    first, final = z == 0, z == nz - 1
    greet("dp", z * 2 + 1 - y)

    @pl.when(jnp.logical_not(first))
    def _():
        greet("dp", (z - 1) * 2 + y)

    @pl.when(jnp.logical_not(final))
    def _():
        greet("dp", (z + 1) * 2 + y)
    each(1, peers, lambda o: greet("tensor", lax.rem(mt + o, peers)))
    each(1, nz, lambda i: first_copy(i).start())
    pl.semaphore_wait(barrier, peers + 2 - jnp.where(first | final, 1, 0))

    def tell(side, step):
        pl.semaphore_signal(token.at[side], inc=1, device_id=beside(step), device_id_type=MESH)

    def chain():
        @pl.when(first)
        def _():
            tell(0, 1)

        @pl.when(final)
        def _():
            tell(1, -1)

        @pl.when(jnp.logical_not(first))
        def _():
            pl.semaphore_wait(token.at[0], 1)

            @pl.when(jnp.logical_not(final))
            def _():
                tell(0, 1)

        @pl.when(jnp.logical_not(final))
        def _():
            pl.semaphore_wait(token.at[1], 1)

            @pl.when(jnp.logical_not(first))
            def _():
                tell(1, -1)
    if nz > 4:
        chain()

    def remote(src, dst, s_sem, r_sem, to):
        return pltpu.make_async_remote_copy(src_ref=src, dst_ref=dst, send_sem=s_sem, recv_sem=r_sem,
                                            device_id={"dp": to}, device_id_type=MESH)

    def loop(body):
        def one(i, _):
            body(pl.ds(pl.multiple_of(i * step, step), step))
            return 0
        lax.fori_loop(0, chunk // step, one, 0)

    def mine(t, d, side, c, at):
        first = pl.multiple_of(c * chunk + at.start, step)
        return raw[t, d * 2 + side, pl.ds(first, step), :].astype(jnp.float32)

    def y_copy(t, d, c, ring):
        s = lax.rem(t, SLOTS)
        return remote(y_cast.at[ring], y_in.at[s, d, c], y_send.at[ring], y_recv.at[d, c], z * 2 + 1 - y)

    def s_copy(t, c):
        s = lax.rem(t, SLOTS)
        return remote(s_out.at[c], s_in.at[s, c], s_send.at[c], s_recv.at[c], z * 2 + 1 - y)

    def z_wait(t, where, c):
        s = lax.rem(t, SLOTS)
        remote(z_in.at[s, where, c], z_in.at[s, where, c], z_send.at[0], z_recv.at[lax.rem(t, 2), where, c], me).wait_recv()

    def landed(t, c):
        for k in range(nz - 2):
            if nz > 4:
                @pl.when((zm <= 1) | (z != k + 1))
                def _():
                    z_wait(t, k, c)
            else:
                z_wait(t, k, c)

    def gathered(t, c, at):
        s = lax.rem(t, SLOTS)
        total = None
        for k in range(nz - 2):
            part = z_in[s, k, c, at, :]
            if nz > 4:
                part = jnp.where((zm <= 1) | (z != k + 1), part, 0.0)
            total = part if total is None else total + part
        return total

    def z_go(t, src, d, c, sem):
        s = lax.rem(t, SLOTS)
        to = jnp.where(is_outer, inner, d)
        where = jnp.where(is_outer, jnp.where(d == inner, d - 1, through(d)), z - 1)
        remote(src, z_in.at[s, where, c], sem, z_recv.at[lax.rem(t, 2), where, c], to * 2 + y).start()

    def z_sent(sem):
        remote(a_cast.at[0, 0], a_cast.at[0, 0], sem, z_recv.at[0, 0, 0], me).wait_send()

    def y_job(t, i, c, ring, full):
        d = order(i)

        @pl.when(full)
        def _():
            y_copy(t, d, c, ring).wait_send()

        def body(at):
            y_cast[ring, at, :] = mine(t, d, 1 - y, c, at)
        loop(body)
        y_copy(t, d, c, ring).start()

    def s_job(t, c):
        @pl.when(t > 0)
        def _():
            s_copy(t, c).wait_send()
        j = n_b(z) + (1 - y) * n_a(z) + c
        landed(t, j)

        def body(at):
            s_out[c, at, :] = gathered(t, j, at) + mine(t, z, 1 - y, n_b(z) + c, at)
        loop(body)
        s_copy(t, c).start()

    def a_job(t, i, j, gone):
        s = lax.rem(t, SLOTS)
        d = order(i)
        side = j // n_a(d)
        c = n_b(d) + lax.rem(j, n_a(d))
        k = n_b(d) + j
        sem = z_send.at[lax.rem(gone, Z_RING)]

        @pl.when(gone >= Z_RING)
        def _():
            z_sent(sem)
        relay = is_inner & (i > 0)

        @pl.when(relay)
        def _():
            w = through(d)
            z_wait(t, w, k)

            def body(at):
                z_in[s, w, k, at, :] = z_in[s, w, k, at, :] + mine(t, d, side, c, at)
            loop(body)
            z_go(t, z_in.at[s, w, k], d, k, sem)

        @pl.when(jnp.logical_not(relay))
        def _():
            def body(at):
                a_cast[i, j, at, :] = mine(t, d, side, c, at)
            loop(body)
            z_go(t, a_cast.at[i, j], d, k, sem)

    def b_job(t, i, c, gone):
        s = lax.rem(t, SLOTS)
        d = order(i)
        sem = z_send.at[lax.rem(gone, Z_RING)]

        @pl.when(gone >= Z_RING)
        def _():
            z_sent(sem)
        y_copy(t, d, c, 0).wait_recv()
        relay = is_inner & (i > 0)

        @pl.when(relay)
        def _():
            w = through(d)
            z_wait(t, w, c)

            def body(at):
                z_in[s, w, c, at, :] = z_in[s, w, c, at, :] + (y_in[s, d, c, at, :] + mine(t, d, y, c, at))
            loop(body)
            z_go(t, z_in.at[s, w, c], d, c, sem)

        @pl.when(jnp.logical_not(relay))
        def _():
            def body(at):
                y_in[s, d, c, at, :] = y_in[s, d, c, at, :] + mine(t, d, y, c, at)
            loop(body)
            z_go(t, y_in.at[s, d, c], d, c, sem)

    def update(t, c, total):
        scale = m_scale[t]
        h = lax.rem(t, 2)

        def fold(x):
            return jnp.max(x.reshape(step // 8, 8, lanes), axis=0)

        def one(it, carry):
            at = pl.ds(pl.multiple_of(it * step, step), step)
            whole = total(at) * (1.0 / n)
            rows_i = pl.ds(pl.multiple_of(c * chunk + it * step, step), step)
            top_m, tops, lows = carry
            new_tops, new_lows = [], []
            for g in range(groups):
                cols = slice(g * lanes, (g + 1) * lanes)
                grad = whole[:, cols]
                m_old = scale * qm[t, rows_i, cols].astype(jnp.float32)
                stored = qv[t, rows_i, cols].astype(jnp.float32)
                inv = 1.0 / jnp.full((1, lanes), v_exp[g, t], jnp.float32)
                v_old = v_max[g, t] * jnp.exp(jnp.log(stored) * inv)
                m = 0.9 * m_old + 0.1 * grad
                v = 0.95 * v_old + 0.05 * grad * grad
                w = par[t, rows_i, cols]
                par[t, rows_i, cols] = w - 0.02 * (m / (jnp.sqrt(v) + 1e-08) + 0.1 * w)
                m_new[h, rows_i, cols] = m
                v_new[h, rows_i, cols] = v
                top_m = jnp.maximum(top_m, fold(jnp.abs(m)))
                new_tops.append(jnp.maximum(tops[g], fold(v)))
                new_lows.append(jnp.maximum(lows[g], fold(-v)))
            return top_m, tuple(new_tops), tuple(new_lows)
        least = jnp.full((8, lanes), -jnp.inf, jnp.float32)
        top_m, tops, lows = lax.fori_loop(0, chunk // step, one, (least, (least,) * groups, (least,) * groups))
        for row, value in enumerate((top_m,) + tops + lows):
            stat[t, row:row + 1, :] = jnp.maximum(stat[t, row:row + 1, :], jnp.max(value, axis=0, keepdims=True))

    def update_a(t, c):
        s = lax.rem(t, SLOTS)

        @pl.when((c == 0) & (t == 0))
        def _():
            for copy in rest[1:]:
                copy.wait()

        @pl.when(c == 0)
        def _():
            stat[t] = jnp.full(stat.shape[1:], -jnp.inf, jnp.float32)
        j = n_b(z) + y * n_a(z) + c
        landed(t, j)
        s_copy(t, c).wait_recv()
        update(t, n_b(z) + c,
               lambda at: gathered(t, j, at) + mine(t, z, y, n_b(z) + c, at) + s_in[s, c, at, :])

    def update_b(t, c):
        s = lax.rem(t, SLOTS)
        y_copy(t, z, c, 0).wait_recv()
        landed(t, c)
        update(t, c, lambda at: gathered(t, c, at) + (y_in[s, z, c, at, :] + mine(t, z, y, c, at)))

    def row_copy(t, o):
        h = t % 2 if isinstance(t, int) else lax.rem(t, 2)
        return pltpu.make_async_remote_copy(
            src_ref=row.at[h], dst_ref=row_in.at[h, o], send_sem=st_send.at[h], recv_sem=st_recv.at[h],
            device_id={"tensor": lax.rem(mt + o // n, peers), "dp": lax.rem(me + lax.rem(o, n), n)},
            device_id_type=MESH)

    def rows_of(t):
        h = lax.rem(t, 2)
        part = row_in.at[h, pl.ds(1, n * peers - 1)]
        return remote(part, part, st_send.at[h], st_recv.at[h], me)

    kinds = stat.shape[1]

    def share(t):
        h = lax.rem(t, 2)
        if not isinstance(t, int) or t >= 2:
            @pl.when(t >= 2)
            def _():
                rows_of(t).wait_send()
        best = jnp.broadcast_to(jnp.max(stat[t], axis=1, keepdims=True), (kinds, lanes))
        at = [lax.broadcasted_iota(jnp.int32, (kinds, lanes), i) for i in range(2)]
        row[h] = jnp.max(jnp.where(at[0] == at[1], best, -jnp.inf), axis=0, keepdims=True)
        if isinstance(t, int):
            for o in reversed(range(1, n * peers)):
                row_copy(t, o).start()
        else:
            each(1, n * peers, lambda o: row_copy(t, n * peers - o).start())

    def all_rows(body):
        def one(i, _):
            body(pl.ds(pl.multiple_of(i * LONG, LONG), LONG))
            return 0
        lax.fori_loop(0, rows // LONG, one, 0)

    def finish(t):
        h = lax.rem(t, 2)
        rows_of(t).wait_recv()
        inverse, exps, invs = merged(n, groups, row, row_in, out_s, t, h)

        def body(at):
            for g in range(groups):
                cols = slice(g * lanes, (g + 1) * lanes)
                value = jnp.exp(exps[g] * jnp.log(v_new[h, at, cols] * invs[g]))
                qv[t, at, cols] = value.astype(jnp.bfloat16)
                qm[t, at, cols] = (m_new[h, at, cols] * inverse).astype(jnp.bfloat16)
        all_rows(body)

    lag_a = jnp.where(is_inner, LAG_A, -LEAD)
    lag_b = jnp.where(is_inner, LAG_B_INNER, LAG_B)
    own = wide * (nz - 1) + sides
    idle = own + wide - n_b(z)

    def place(g, lag):
        g = g - lag
        ok = (g >= 0) & (g < count * period)
        g = jnp.clip(g, 0, count * period - 1)
        return ok, g // period, lax.rem(g, period)

    def one(it, carry):
        sent, gone = carry
        g = it - LEAD
        ok, t, p = place(g, -LEAD)

        @pl.when(ok & (t == 0) & (p == 0))
        def _():
            first_copy(0, 0, nz).wait()

        @pl.when(ok & (t == 0) & (p == LEAD + 2))
        def _():
            for c in rest:
                c.start()
            each(1, nz, lambda i: first_copy(i).wait())

        if nz == 4:
            @pl.when(g == CHAIN_AT)
            def _():
                chain()

        @pl.when(ok & (t == 1) & (p == 0))
        def _():
            rest[0].wait()

        ok, t, p = place(g, 0)
        tail = p >= own
        i = jnp.where(tail, nz - 1, p // wide)
        c = jnp.where(tail, p - idle, lax.rem(p, wide))
        live = ok & (tail | (p < own - sides)) & (c >= 0) & (c < n_b(order(i)))

        @pl.when(live)
        def _():
            y_job(t, i, c, lax.rem(sent, RING), sent >= RING)
        sent = sent + jnp.where(live, 1, 0)
        c = p - (own - sides)

        @pl.when(ok & (c >= 0) & (c < n_a(z)) & (p < own))
        def _():
            s_job(t, c)

        @pl.when(g == 0)
        def _():
            first_copy(0, chunk).wait()

        ok, t, p = place(g, lag_a)
        i, j = jnp.minimum(p // tall, nz - 2), lax.rem(p, tall)

        live = ok & (p < tall * (nz - 1)) & (j < 2 * n_a(order(i)))

        @pl.when(live)
        def _():
            a_job(t, i, j, gone)
        gone = gone + jnp.where(live, 1, 0)

        ok, t, p = place(g, lag_b)
        i, c = p // wide, lax.rem(p, wide)

        live = ok & (p < own - sides) & (c < n_b(order(i)))

        @pl.when(live)
        def _():
            b_job(t, i, c, gone)
        gone = gone + jnp.where(live, 1, 0)

        ok, t, p = place(g, LAG_UPDATE)
        c = p - (own - sides)

        @pl.when(ok & (c >= 0) & (c < n_a(z)) & (p < own))
        def _():
            update_a(t, c)
        c = p - idle

        @pl.when(ok & (c >= 0) & (p >= own))
        def _():
            update_b(t, c)

        @pl.when(ok & (p == period - 1) & (t < count - 1))
        def _():
            share(t)

        ok, t, p = place(g, LAG_UPDATE + LAG_FINISH)

        @pl.when(ok & (p == period - 1))
        def _():
            finish(t)
        return sent, gone

    lax.fori_loop(0, LEAD + count * period + LAG_UPDATE, one, (0, 0))
    share(count - 1)

    each(0, RING, lambda r: y_copy(0, 0, 0, r).wait_send())
    each(0, Z_RING, lambda r: z_sent(z_send.at[r]))
    each(0, n_a(z), lambda c: s_copy(0, c).wait_send())
    for t in range(max(0, count - 2), count):
        rows_of(t).wait_send()
    rows_of(count - 1).wait_recv()


def last(n, par, qm, qv, m_new, v_new, old, row, row_in, out_p, out_m, out_v, out_scale, out_top, out_exp,
         qm_last, qv_last, stats, scale, top, exp, sem):
    count, rows, width = par.shape
    groups = out_top.shape[0]
    lanes = width // groups
    t = count - 1
    h = t % 2
    copies = [pltpu.make_async_copy(par, out_p, sem.at[0])]
    for i, (src, dst) in enumerate(((qm, out_m), (qv, out_v))):
        copies.append(pltpu.make_async_copy(src.at[pl.ds(0, t)], dst.at[pl.ds(0, t)], sem.at[1 + i]))
    for c in copies:
        c.start()
    stats[pl.ds(0, t)] = old[pl.ds(0, t)]
    inverse, exps, invs = merged(n, groups, row, row_in, stats, t, h)
    lane = lax.broadcasted_iota(jnp.int32, (1, lanes), 1)

    def packed(k):
        line = stats[0, k:k + 1, :]
        for u in range(1, count):
            line = jnp.where(lane == u, stats[u, k:k + 1, :], line)
        return line[:, :count]
    scale[...] = packed(0)
    for g in range(groups):
        top[g:g + 1, :] = packed(1 + g)
        exp[g:g + 1, :] = packed(1 + groups + g)
    for i, (src, dst) in enumerate(((scale, out_scale), (top, out_top), (exp, out_exp))):
        c = pltpu.make_async_copy(src, dst, sem.at[3 + i])
        c.start()
        copies.append(c)

    def body(i, _):
        at = pl.ds(pl.multiple_of(i * LONG, LONG), LONG)
        for g in range(groups):
            cols = slice(g * lanes, (g + 1) * lanes)
            value = jnp.exp(exps[g] * jnp.log(v_new[h, at, cols] * invs[g]))
            qv_last[at, cols] = value.astype(jnp.bfloat16)
            qm_last[at, cols] = (m_new[h, at, cols] * inverse).astype(jnp.bfloat16)
        return 0
    lax.fori_loop(0, rows // LONG, body, 0)
    for i, (src, dst) in enumerate(((qm_last, out_m), (qv_last, out_v))):
        c = pltpu.make_async_copy(src, dst.at[t], sem.at[6 + i])
        c.start()
        copies.append(c)
    for c in copies:
        c.wait()


def on_device(n, peers, grads, param, q_m, m_scale, q_v, v_max, v_exp):
    count, rows, width = q_m.shape
    groups = v_max.shape[1]
    lanes = width // groups
    nz = n // 2
    chunk = rows // (8 * SPLIT)
    wide, tall, deep = 7 * SPLIT, 4 * SPLIT, 10 * SPLIT
    kinds = -(-(1 + 2 * groups) // 8) * 8
    f32, bf16 = jnp.float32, jnp.bfloat16
    dma = pltpu.SemaphoreType.DMA
    hbm = pl.BlockSpec(memory_space=pl.ANY)
    smem = pl.BlockSpec(memory_space=pltpu.SMEM)
    vmem = pl.BlockSpec(memory_space=pltpu.VMEM)
    buffers = [
        pltpu.VMEM((count, n, rows, width), bf16),
        pltpu.VMEM((RING, chunk, width), f32),
        pltpu.VMEM((nz - 1, tall, chunk, width), f32),
        pltpu.VMEM((SLOTS, nz, wide, chunk, width), f32),
        pltpu.VMEM((SLOTS, 2 * (nz - 2), deep, chunk, width), f32),
        pltpu.VMEM((2 * SPLIT, chunk, width), f32),
        pltpu.VMEM((SLOTS, 2 * SPLIT, chunk, width), f32),
        pltpu.VMEM((count, kinds, lanes), f32),
    ]
    grant = SPARE + sum(math.prod(b.shape) * b.dtype.itemsize for b in buffers)
    state = pl.pallas_call(
        functools.partial(kernel, n, peers),
        out_shape=(
            pltpu.VMEM(param.shape, f32),
            pltpu.VMEM(q_m.shape, bf16),
            pltpu.VMEM(q_v.shape, bf16),
            pltpu.VMEM((2, rows, width), f32),
            pltpu.VMEM((2, rows, width), f32),
            pltpu.VMEM((count, kinds, lanes), f32),
            pltpu.VMEM((2, 1, lanes), f32),
            pltpu.VMEM((2, n * peers, 1, lanes), f32),
        ),
        in_specs=[hbm] * 4 + [smem] * 3,
        out_specs=[vmem] * 8,
        scratch_shapes=buffers + [
            dma((nz + 1,)), dma((4,)), pltpu.SemaphoreType.REGULAR((2,)),
            dma((RING,)), dma((nz, wide)),
            dma((Z_RING,)), dma((2, 2 * (nz - 2), deep)),
            dma((2 * SPLIT,)), dma((2 * SPLIT,)),
            dma((2,)), dma((2,)),
        ],
        compiler_params=pltpu.CompilerParams(
            collective_id=0, has_side_effects=True, vmem_limit_bytes=grant
        ),
    )(grads[0].reshape(count, n, rows, width), param, q_m, q_v, m_scale, v_max.T, v_exp.T)
    new_param, new_q_m, new_q_v, scales, tops, exps = pl.pallas_call(
        functools.partial(last, n),
        out_shape=(
            jax.ShapeDtypeStruct(param.shape, f32),
            jax.ShapeDtypeStruct(q_m.shape, bf16),
            jax.ShapeDtypeStruct(q_v.shape, bf16),
            jax.ShapeDtypeStruct((1, count), f32),
            jax.ShapeDtypeStruct((groups, count), f32),
            jax.ShapeDtypeStruct((groups, count), f32),
        ),
        in_specs=[vmem] * 8,
        out_specs=[hbm] * 6,
        scratch_shapes=[
            pltpu.VMEM((rows, width), bf16),
            pltpu.VMEM((rows, width), bf16),
            pltpu.VMEM((count, kinds, lanes), f32),
            pltpu.VMEM((1, count), f32),
            pltpu.VMEM((groups, count), f32),
            pltpu.VMEM((groups, count), f32),
            dma((8,)),
        ],
        compiler_params=pltpu.CompilerParams(vmem_limit_bytes=4 << 20),
    )(*state)
    return new_param, new_q_m, scales.reshape(count), new_q_v, tops.T, exps.T


def solution(mesh):
    in_specs = (
        P("dp", None, None, "tensor"),
        P(None, "dp", "tensor"),
        P(None, "dp", "tensor"),
        P(),
        P(None, "dp", "tensor"),
        P(None, "tensor"),
        P(None, "tensor"),
    )
    out_specs = (
        P(None, "dp", "tensor"),
        P(None, "dp", "tensor"),
        P(),
        P(None, "dp", "tensor"),
        P(None, "tensor"),
        P(None, "tensor"),
    )
    return jax.shard_map(
        functools.partial(on_device, mesh.shape["dp"], mesh.shape["tensor"]),
        mesh=mesh, in_specs=in_specs, out_specs=out_specs, check_vma=False
    )
```
